32 devices in a mesh: pp: 4 (over z), dp: 8 (over y, x, core).
Axes of the slice: x: 2, y: 2, z: 4, core: 2. Of those that a mesh axis runs over, the one named last changes fastest.
Arguments:
- w_in: bfloat16 [4, 2, 768, 3072], P('pp')
- w_out: bfloat16 [4, 2, 3072, 768], P('pp')
- x_saved: bfloat16 [4, 4, 2, 512, 768], P('pp', None, None, 'dp')
- h_saved: bfloat16 [4, 4, 2, 512, 3072], P('pp', None, None, 'dp')
- dy_in: bfloat16 [4, 512, 768], P('pp', 'dp')
- acc_in: float32 [4, 8, 2, 768, 3072], P('pp', 'dp')
- acc_out: float32 [4, 8, 2, 3072, 768], P('pp', 'dp')
Outputs:
- output 1: float32 [4, 2, 768, 3072], P('pp')
- output 2: float32 [4, 2, 3072, 768], P('pp')
- output 3: bfloat16 [4, 512, 768], P('pp', 'dp')
All inputs are finite; a program needn't handle non-finite values.
Results may differ from the reference program's by a relative error of at most 0.0112023.
Values are sent between devices in bfloat16 or wider.
A program may use at most 1 GiB of HBM per device.

```python
import jax
import jax.numpy as jnp
from jax import lax

STAGES = 4
REPLICAS = 8
LAYERS_STAGE = 2
TOKENS_DEV = 64
HIDDEN = 768
FF_WIDTH = 3072

ROWS = REPLICAS * TOKENS_DEV
TOTAL_DEPTH = STAGES * LAYERS_STAGE


def setup_inputs(seed: int = 0) -> dict:
    key_list = jax.random.split(jax.random.key(seed), 7)
    tok_factor = TOKENS_DEV ** 0.5
    pending = (STAGES - jnp.arange(STAGES)).astype(jnp.float32)
    scale_in = jnp.sqrt(pending * tok_factor / (8.0 * TOTAL_DEPTH)).reshape(STAGES, 1, 1, 1, 1)
    scale_out = (0.65 * jnp.sqrt(pending * tok_factor)).reshape(STAGES, 1, 1, 1, 1)
    w_in = jax.random.normal(key_list[0], (STAGES, LAYERS_STAGE, HIDDEN, FF_WIDTH), jnp.float32) * HIDDEN ** -0.5
    w_out = jax.random.normal(key_list[1], (STAGES, LAYERS_STAGE, FF_WIDTH, HIDDEN), jnp.float32) * (FF_WIDTH * TOTAL_DEPTH) ** -0.5
    x_saved = jax.random.normal(key_list[2], (STAGES, STAGES, LAYERS_STAGE, ROWS, HIDDEN), jnp.float32)
    h_saved = jax.random.normal(key_list[3], (STAGES, STAGES, LAYERS_STAGE, ROWS, FF_WIDTH), jnp.float32)
    dy_in = jax.random.normal(key_list[4], (STAGES, ROWS, HIDDEN), jnp.float32) * TOKENS_DEV ** -0.25
    acc_in = jax.random.normal(key_list[5], (STAGES, REPLICAS, LAYERS_STAGE, HIDDEN, FF_WIDTH), jnp.float32) * scale_in
    acc_out = jax.random.normal(key_list[6], (STAGES, REPLICAS, LAYERS_STAGE, FF_WIDTH, HIDDEN), jnp.float32) * scale_out
    return {'w_in': w_in.astype(jnp.bfloat16), 'w_out': w_out.astype(jnp.bfloat16), 'x_saved': x_saved.astype(jnp.bfloat16), 'h_saved': h_saved.astype(jnp.bfloat16), 'dy_in': dy_in.astype(jnp.bfloat16), 'acc_in': acc_in, 'acc_out': acc_out}


def layer_backward(w_first, w_second, x_in, h_pre, cot_in):
    act_val, act_vjp = jax.vjp(jax.nn.gelu, h_pre.astype(jnp.float32))
    act_bf = act_val.astype(jnp.bfloat16)
    d_act = jnp.dot(cot_in, w_second.T, preferred_element_type=jnp.float32)
    d_pre = act_vjp(d_act)[0].astype(jnp.bfloat16)
    x_rows = x_in.reshape(REPLICAS, TOKENS_DEV, HIDDEN).astype(jnp.float32)
    pre_rows = d_pre.reshape(REPLICAS, TOKENS_DEV, FF_WIDTH).astype(jnp.float32)
    act_rows = act_bf.reshape(REPLICAS, TOKENS_DEV, FF_WIDTH).astype(jnp.float32)
    cot_rows = cot_in.reshape(REPLICAS, TOKENS_DEV, HIDDEN).astype(jnp.float32)
    grad_first = jnp.einsum('rtd,rtf->rdf', x_rows, pre_rows)
    grad_second = jnp.einsum('rtf,rtd->rfd', act_rows, cot_rows)
    back_sum = jnp.dot(d_pre, w_first.T, preferred_element_type=jnp.float32)
    cot_out = (cot_in.astype(jnp.float32) + back_sum).astype(jnp.bfloat16)
    return cot_out, grad_first, grad_second


def stage_backward(w_first, w_second, x_stage, h_stage, cot_in):
    def layer_body(cot_carry, layer_data):
        cot_next, grad_first, grad_second = layer_backward(layer_data[0], layer_data[1], layer_data[2], layer_data[3], cot_carry)
        return cot_next, (grad_first, grad_second)
    cot_out, grad_stack = lax.scan(layer_body, cot_in, (w_first, w_second, x_stage, h_stage), reverse=True)
    return cot_out, grad_stack[0], grad_stack[1]


def reference(w_in, w_out, x_saved, h_saved, dy_in, acc_in, acc_out):
    def stage_body(step_id, loop_state):
        cot_stack, grad_in, grad_out = loop_state
        stage_id = STAGES - 1 - step_id
        cot_stack = lax.dynamic_update_index_in_dim(cot_stack, dy_in[stage_id], stage_id, 0)
        w_first = w_in[stage_id]
        w_second = w_out[stage_id]
        x_stage = x_saved[stage_id]
        h_stage = h_saved[stage_id]

        def micro_body(slot_id, inner_state):
            cot_list, acc_first, acc_second = inner_state
            micro_id = stage_id + slot_id
            cot_out, grad_first, grad_second = stage_backward(w_first, w_second, x_stage[slot_id], h_stage[slot_id], cot_list[micro_id])
            cot_list = lax.dynamic_update_index_in_dim(cot_list, cot_out, micro_id, 0)
            return cot_list, acc_first + jnp.swapaxes(grad_first, 0, 1), acc_second + jnp.swapaxes(grad_second, 0, 1)

        cot_stack, acc_first, acc_second = lax.fori_loop(0, STAGES - stage_id, micro_body, (cot_stack, acc_in[stage_id], acc_out[stage_id]))
        mean_first = jnp.sum(acc_first.astype(jnp.bfloat16).astype(jnp.float32), axis=0) / REPLICAS
        mean_second = jnp.sum(acc_second.astype(jnp.bfloat16).astype(jnp.float32), axis=0) / REPLICAS
        grad_in = lax.dynamic_update_index_in_dim(grad_in, mean_first, stage_id, 0)
        grad_out = lax.dynamic_update_index_in_dim(grad_out, mean_second, stage_id, 0)
        return cot_stack, grad_in, grad_out

    start_state = (jnp.zeros((STAGES, ROWS, HIDDEN), jnp.bfloat16), jnp.zeros((STAGES, LAYERS_STAGE, HIDDEN, FF_WIDTH), jnp.float32), jnp.zeros((STAGES, LAYERS_STAGE, FF_WIDTH, HIDDEN), jnp.float32))
    cot_stack, grad_in, grad_out = lax.fori_loop(0, STAGES, stage_body, start_state)
    return grad_in, grad_out, cot_stack
```

```python
import functools
import jax
import jax.numpy as jnp
from jax import lax
from jax.experimental import pallas as pl
from jax.experimental.pallas import tpu as pltpu
from jax.sharding import PartitionSpec as P

BF16 = jnp.bfloat16
F32 = jnp.float32
NT = (((1,), (1,)), ((), ()))
COLS = 2
RING = 4


def gelu_and_slope(h):
    root = 0.7978845608028654
    cube = 0.044715
    sq = h * h
    th = jnp.tanh(root * (h + cube * (h * sq)))
    cdf = 0.5 * (1.0 + th)
    slope = cdf + (0.5 * root) * h * (1.0 - th * th) * (1.0 + (3.0 * cube) * sq)
    return h * cdf, slope


def main_kernel(sizes, w_in, w_out, x_saved, h_saved, dy_in, acc_in, acc_out,
                m_ref, dx_ref,
                wi_s, wo_s, lt_s, rm_s, xs_s, cb_s, acc_s, p_s, h1_s, h2_s,
                wsem, hsem, xsem, dysem, accsem, cot_send, cot_recv, dx_send, dx_recv, dx_loc,
                send_sem, recv_sem, free_sem):
    hid, ff, tok, stages = sizes
    cw = hid // COLS
    nq = ff // cw
    per_kind = nq
    per_layer = 2 * nq
    total = 2 * per_layer
    nblk = ff // hid
    unit = hid // 16
    rows4 = stages * tok

    pp = lax.axis_index('pp')
    dp = lax.axis_index('dp')
    core = dp % 2
    xc = (dp // 2) % 2
    yc = dp // 4
    pair = dp + 1 - 2 * core
    xn = dp + 2 - 4 * xc
    yn = dp + 4 - 8 * yc

    def dev(pp_i, dp_i):
        return dict(device_id=(pp_i, dp_i), device_id_type=pl.DeviceIdType.MESH)

    def w_copy(k, which):
        if which == 0:
            return [pltpu.make_async_copy(w_out.at[0, k], wo_s.at[k], wsem.at[k, 0])]
        return [pltpu.make_async_copy(w_in.at[0, k, :, pl.ds(q * cw, cw)], wi_s.at[k, q], wsem.at[k, 1 + q]) for q in range(nq)]

    def h_copy(k, t, q):
        return pltpu.make_async_copy(h_saved.at[0, t, k, :, pl.ds(pl.multiple_of(q * cw, 128), cw)],
                                     rm_s.at[k, COLS + q, pl.ds(pl.multiple_of(t * tok, tok), tok), :], hsem.at[k, t, q])

    def x_copy():
        return pltpu.make_async_copy(x_saved.at[0], xs_s, xsem)

    dy_copy = pltpu.make_async_copy(dy_in.at[0], cb_s.at[0], dysem)

    def acc_where(c):
        k = 1 - c // per_layer
        b = c % per_layer
        return k, b // per_kind, b % per_kind

    def acc_copies(c):
        k, kind, jj = acc_where(c)
        slot = c % 2
        a = pltpu.make_async_copy(acc_out.at[0, 0, k, pl.ds(pl.multiple_of((jj // COLS) * hid, 128), hid), pl.ds(pl.multiple_of((jj % COLS) * cw, 128), cw)],
                                  acc_s.at[slot], accsem.at[slot])
        b = pltpu.make_async_copy(acc_in.at[0, 0, k, :, pl.ds(pl.multiple_of(jj * cw, 128), cw)], acc_s.at[slot], accsem.at[slot])
        return kind, a, b

    def acc_start(c):
        kind, a, b = acc_copies(c)

        @pl.when(kind == 0)
        def _():
            a.start()

        @pl.when(kind == 1)
        def _():
            b.start()

    def acc_wait(c):
        acc_copies(c)[2].wait()

    dy_copy.start()
    for k in (1, 0):
        for q in range(nq):
            h_copy(k, 0, q).start()
        for which in (0, 1):
            for cp in w_copy(k, which):
                cp.start()
    x_copy().start()

    def h_rest(i, carry):
        k = 1 - i % 2
        t = 1 + i // 2
        for q in range(nq):
            h_copy(k, t, q).start()
        return carry

    lax.fori_loop(0, 2 * (stages - 1), h_rest, 0)
    acc_start(0)

    barrier = pltpu.get_barrier_semaphore()
    for other in (pair, xn, yn):
        pl.semaphore_signal(barrier, inc=1, **dev(pp, other))
    for step in range(1, stages):
        pl.semaphore_signal(barrier, inc=1, **dev((pp + step) % stages, dp))
    pl.semaphore_wait(barrier, 3 + stages - 1)

    def cot_copy(t):
        return pltpu.make_async_remote_copy(src_ref=cb_s.at[t], dst_ref=cb_s.at[t + 1], send_sem=cot_send.at[t], recv_sem=cot_recv.at[t + 1],
                                            **dev(jnp.maximum(pp - 1, 0), dp))

    def cot_arrival(t):
        return pltpu.make_async_remote_copy(src_ref=cb_s.at[t], dst_ref=cb_s.at[t], send_sem=cot_send.at[0], recv_sem=cot_recv.at[t],
                                            **dev(jnp.maximum(pp - 1, 0), dp))

    def dx_copy(t):
        return pltpu.make_async_remote_copy(src_ref=cb_s.at[t], dst_ref=dx_ref.at[0], send_sem=dx_send.at[t], recv_sem=dx_recv,
                                            **dev(t, dp))

    def layer(t, k, cot):
        rows = pl.ds(pl.multiple_of(t * tok, tok), tok)
        for j in range(COLS):
            rm_s[k, j, rows, :] = cot[:, j * cw:(j + 1) * cw]
        back = cot.astype(F32)
        for q in range(nq):
            e = lax.dot_general(cot, wo_s[k, q * cw:(q + 1) * cw, :], NT, preferred_element_type=F32)
            _, slope = gelu_and_slope(rm_s[k, COLS + q, rows, :].astype(F32))
            dh = (e * slope).astype(BF16)
            rm_s[k, COLS + q, rows, :] = dh
            back += lax.dot_general(dh, wi_s[k, q], NT, preferred_element_type=F32)
        return back.astype(BF16)

    def prepare(half):
        cols = pl.ds(half * 2 * tok, 2 * tok)

        def one_layer(k, carry):
            xx = jnp.concatenate([xs_s[2 * half, k], xs_s[2 * half + 1, k]], axis=0)
            lt_s[k, 0, :, cols] = xx.T
            return carry

        lax.fori_loop(0, 2, one_layer, 0)

    def chain_step(t, carry):
        active = pp + t < stages

        first = isinstance(t, int)
        if first:
            dy_copy.wait()
        else:
            @pl.when(active)
            def _():
                cot_arrival(t).wait_recv()

        @pl.when(active)
        def _():
            def one(i, cot_idx):
                k = 1 - i

                if first:
                    for which in (0, 1):
                        for cp in w_copy(k, which):
                            cp.wait()
                cot = cb_s[t]
                out = layer(t, k, cot)
                cb_s[t] = out
                return cot_idx
            lax.fori_loop(0, 2, one, 0)

            @pl.when(pp > 0)
            def _():
                cot_copy(t).start()

            if not first:
                @pl.when(pp == 0)
                def _():
                    dx_copy(t).start()

        return carry

    def h_wait(i, carry):
        for q in range(nq):
            h_copy(1 - i % 2, i // 2, q).wait()
        return carry

    def zero_inactive(t, carry):
        @pl.when(pp + t >= stages)
        def _():
            rows = pl.ds(pl.multiple_of(t * tok, tok), tok)
            zero = jnp.zeros((tok, cw), BF16)

            def one_layer(k, c2):
                for j in range(COLS + nq):
                    rm_s[k, j, rows, :] = zero
                return c2
            lax.fori_loop(0, 2, one_layer, 0)
        return carry

    def acts(half):
        def body(i, carry):
            k = 1 - i // nq
            q = i % nq
            cols = pl.ds(half * 2 * tok, 2 * tok)
            hh = rm_s[k, COLS + q, pl.ds(half * 2 * tok, 2 * tok), :].astype(F32)
            act, _ = gelu_and_slope(hh)
            lt_s[k, 1 + q // COLS, pl.ds(pl.multiple_of((q % COLS) * cw, 128), cw), cols] = act.astype(BF16).T
            return carry
        lax.fori_loop(0, 2 * nq, body, 0)

    lax.fori_loop(0, 4, h_wait, 0)
    acts(0)
    chain_step(0, 0)
    lax.fori_loop(4, 2 * stages, h_wait, 0)
    x_copy().wait()
    for half in range(1, stages // 2):
        acts(half)
    for half in range(stages // 2):
        prepare(half)
    lax.fori_loop(1, stages, zero_inactive, 0)
    lax.fori_loop(1, stages, chain_step, 0)

    half = hid // 2
    hb = core * half
    xb = hb
    yb = hb + 4 * unit

    def rows_of(start, n):
        return pl.ds(pl.multiple_of(start, 16), n)

    def remote(kind, c, src, dst, target):
        return pltpu.make_async_remote_copy(src_ref=src, dst_ref=dst, send_sem=send_sem.at[kind, c % RING], recv_sem=recv_sem.at[kind, c], **dev(pp, target))

    def msg(kind, c, arriving=False):
        f = 1 if arriving else 0
        if kind == 0:
            other = m_ref.at[c, rows_of(half - hb, half), :]
            return remote(0, c, other, p_s.at[c], pair)
        if kind == 1:
            return remote(1, c, p_s.at[c, rows_of((1 - xc) * 2 * unit, 2 * unit), :], h1_s.at[c, 0], xn)
        if kind == 2:
            return remote(2, c, p_s.at[c, rows_of(4 * unit + (1 - yc) * 2 * unit, 2 * unit), :], h1_s.at[c, 1], yn)
        if kind == 3:
            return remote(3, c, h1_s.at[c, 0, rows_of((1 - yc) * unit, unit), :], h2_s.at[c, 0], yn)
        if kind == 4:
            return remote(4, c, h1_s.at[c, 1, rows_of((1 - xc) * unit, unit), :], h2_s.at[c, 1], xn)
        if kind == 5:
            y_of = 1 - yc if f else yc
            r = m_ref.at[c, rows_of(xb + xc * 2 * unit + y_of * unit, unit), :]
            return remote(5, c, r, r, yn)
        if kind == 6:
            x_of = 1 - xc if f else xc
            r = m_ref.at[c, rows_of(yb + yc * 2 * unit + x_of * unit, unit), :]
            return remote(6, c, r, r, xn)
        if kind == 7:
            x_of = 1 - xc if f else xc
            r = m_ref.at[c, rows_of(xb + x_of * 2 * unit, 2 * unit), :]
            return remote(7, c, r, r, xn)
        if kind == 8:
            y_of = 1 - yc if f else yc
            r = m_ref.at[c, rows_of(yb + y_of * 2 * unit, 2 * unit), :]
            return remote(8, c, r, r, yn)
        base = half - hb if f else hb
        r = m_ref.at[c, rows_of(base, half), :]
        return remote(9, c, r, r, pair)

    def send(kind, c):
        if kind > 0:
            @pl.when(c >= RING)
            def _():
                msg(kind, c - RING).wait_send()
        msg(kind, c).start()

    def arrive(kind, c):
        msg(kind, c, True).wait_recv()

    def plus(left, right):
        return (left.astype(F32) + right.astype(F32)).astype(BF16)

    def produce(c):
        @pl.when(c + 1 < total)
        def _():
            acc_start(c + 1)
        acc_wait(c)
        k, kind, jj = acc_where(c)
        li = (1 - kind) * (1 + jj // COLS)
        ri = (1 - kind) * (jj % COLS) + kind * (COLS + jj)
        slot = c % 2
        nr = hid // 6 if hid % 768 == 0 else hid // 2
        for i in range(hid // nr):
            r = pl.ds(i * nr, nr)
            g = jnp.dot(lt_s[k, li, r, :], rm_s[k, ri], preferred_element_type=F32)
            m_ref[c, r, :] = (acc_s[slot, r, :] + g).astype(BF16)
        send(0, c)

    def stage1(c):
        arrive(0, c)
        p_s[c] = plus(p_s[c], m_ref[c, rows_of(hb, half), :])
        send(1, c)
        send(2, c)
        msg(0, c).wait_send()
        pl.semaphore_signal(free_sem, inc=1, **dev(pp, pair))

    def stage2(c):
        arrive(1, c)
        h1_s[c, 0] = plus(h1_s[c, 0], p_s[c, rows_of(xc * 2 * unit, 2 * unit), :])
        send(3, c)
        arrive(2, c)
        h1_s[c, 1] = plus(h1_s[c, 1], p_s[c, rows_of(4 * unit + yc * 2 * unit, 2 * unit), :])
        send(4, c)

    def stage3(c):
        arrive(3, c)
        m_ref[c, rows_of(xb + xc * 2 * unit + yc * unit, unit), :] = plus(h1_s[c, 0, rows_of(yc * unit, unit), :], h2_s[c, 0])
        send(5, c)
        arrive(4, c)
        m_ref[c, rows_of(yb + yc * 2 * unit + xc * unit, unit), :] = plus(h1_s[c, 1, rows_of(xc * unit, unit), :], h2_s[c, 1])
        send(6, c)

    def stage4(c):
        arrive(5, c)
        send(7, c)
        arrive(6, c)
        send(8, c)

    def stage5(c):
        arrive(7, c)
        arrive(8, c)
        pl.semaphore_wait(free_sem, 1)
        send(9, c)

    def stage6(c):
        arrive(9, c)

    plan = ((stage6, 9), (stage5, 8), (stage4, 6), (stage3, 5), (stage2, 3), (stage1, 1), (produce, 0))
    depth = max(lag for _, lag in plan)

    def run(i, carry):
        for fn, lag in plan:
            c = i - lag

            @pl.when((c >= 0) & (c < total))
            def _():
                fn(c)
        return carry

    lax.fori_loop(0, total + depth, run, 0)

    def drain(i, carry):
        for kind in range(1, 10):
            msg(kind, total - RING + i).wait_send()
        return carry

    lax.fori_loop(0, RING, drain, 0)

    @pl.when(pp == 0)
    def _():
        own = pltpu.make_async_copy(cb_s.at[0], dx_ref.at[0], dx_loc)
        own.start()
        own.wait()

        def sent(t, carry):
            dx_copy(t).wait_send()
            return carry
        lax.fori_loop(1, stages, sent, 0)

    @pl.when(pp > 0)
    def _():
        dx_copy(0).wait_recv()

        def sent(t, carry):
            cot_copy(t).wait_send()
            return carry
        lax.fori_loop(0, stages - pp, sent, 0)


def write_kernel(sizes, m_ref, gi_ref, go_ref, out_s, out_sem):
    hid, ff, tok, stages = sizes
    cw = hid // COLS
    nq = ff // cw
    per_layer = 2 * nq
    total = 2 * per_layer
    slots = out_s.shape[0]

    def copies(c):
        k = 1 - c // per_layer
        b = c % per_layer
        kind, jj = b // nq, b % nq
        slot = c % slots
        a = pltpu.make_async_copy(out_s.at[slot], go_ref.at[0, k, pl.ds(pl.multiple_of((jj // COLS) * hid, 128), hid), pl.ds(pl.multiple_of((jj % COLS) * cw, 128), cw)], out_sem.at[slot])
        b = pltpu.make_async_copy(out_s.at[slot], gi_ref.at[0, k, :, pl.ds(pl.multiple_of(jj * cw, 128), cw)], out_sem.at[slot])
        return kind, a, b

    def body(c, carry):
        @pl.when(c >= slots)
        def _():
            copies(c - slots)[2].wait()
        slot = c % slots
        nr = hid // 4
        for i in range(4):
            r = pl.ds(i * nr, nr)
            out_s[slot, r, :] = m_ref[c, r, :].astype(F32) * 0.125
        kind, a, b = copies(c)

        @pl.when(kind == 0)
        def _():
            a.start()

        @pl.when(kind == 1)
        def _():
            b.start()
        return carry

    lax.fori_loop(0, total, body, 0)

    def drain(i, carry):
        copies(total - slots + i)[2].wait()
        return carry
    lax.fori_loop(0, slots, drain, 0)


def solution(mesh):
    stages = mesh.shape['pp']

    def device_fn(w_in, w_out, x_saved, h_saved, dy_in, acc_in, acc_out):
        hid, ff = w_in.shape[2:]
        tok = dy_in.shape[1]
        sizes = (hid, ff, tok, stages)
        cw = hid // COLS
        nq = ff // cw
        total = 4 * nq
        unit = hid // 16
        any_spec = pl.BlockSpec(memory_space=pltpu.HBM)
        vm_spec = pl.BlockSpec(memory_space=pltpu.VMEM)
        m_all, dx = pl.pallas_call(
            functools.partial(main_kernel, sizes),
            out_shape=(pltpu.VMEM((total, hid, cw), BF16), jax.ShapeDtypeStruct((1, tok, hid), BF16)),
            in_specs=[any_spec] * 7,
            out_specs=(vm_spec, vm_spec),
            scratch_shapes=[
                pltpu.VMEM((2, nq, hid, cw), BF16),
                pltpu.VMEM((2, ff, hid), BF16),
                pltpu.VMEM((2, 1 + ff // hid, hid, stages * tok), BF16),
                pltpu.VMEM((2, COLS + nq, stages * tok, cw), BF16),
                pltpu.VMEM((stages, 2, tok, hid), BF16),
                pltpu.VMEM((stages, tok, hid), BF16),
                pltpu.VMEM((2, hid, cw), F32),
                pltpu.VMEM((total, hid // 2, cw), BF16),
                pltpu.VMEM((total, 2, 2 * unit, cw), BF16),
                pltpu.VMEM((total, 2, unit, cw), BF16),
                pltpu.SemaphoreType.DMA((2, 1 + nq)),
                pltpu.SemaphoreType.DMA((2, stages, nq)),
                pltpu.SemaphoreType.DMA,
                pltpu.SemaphoreType.DMA,
                pltpu.SemaphoreType.DMA((2,)),
                pltpu.SemaphoreType.DMA((stages,)),
                pltpu.SemaphoreType.DMA((stages,)),
                pltpu.SemaphoreType.DMA((stages,)),
                pltpu.SemaphoreType.DMA,
                pltpu.SemaphoreType.DMA,
                pltpu.SemaphoreType.DMA((10, RING)),
                pltpu.SemaphoreType.DMA((10, total)),
                pltpu.SemaphoreType.REGULAR,
            ],
            compiler_params=pltpu.CompilerParams(collective_id=0, has_side_effects=True, vmem_limit_bytes=46720 * 1024),
            name='chain_reduce',
        )(w_in, w_out, x_saved, h_saved, dy_in, acc_in, acc_out)
        grad_in, grad_out = pl.pallas_call(
            functools.partial(write_kernel, sizes),
            out_shape=(jax.ShapeDtypeStruct((1, 2, hid, ff), F32), jax.ShapeDtypeStruct((1, 2, ff, hid), F32)),
            in_specs=[vm_spec],
            out_specs=(any_spec, any_spec),
            scratch_shapes=[pltpu.VMEM((4, hid, cw), F32), pltpu.SemaphoreType.DMA((4,))],
            compiler_params=pltpu.CompilerParams(vmem_limit_bytes=16 * 1024 * 1024),
            name='write_out',
        )(m_all)
        return grad_in, grad_out, dx

    return jax.shard_map(device_fn, mesh=mesh, in_specs=(P('pp'), P('pp'), P('pp', None, None, 'dp'), P('pp', None, None, 'dp'), P('pp', 'dp'), P('pp', 'dp'), P('pp', 'dp')), out_specs=(P('pp'), P('pp'), P('pp', 'dp')), check_vma=False)
```

```python
import functools
import jax
import jax.numpy as jnp
from jax import lax
from jax.experimental import pallas as pl
from jax.experimental.pallas import tpu as pltpu
from jax.sharding import PartitionSpec as P

BF16 = jnp.bfloat16
F32 = jnp.float32
NT = (((1,), (1,)), ((), ()))
COLS = 2
TILES = 3
RING = 4
RECV_RING = 8
EARLY = 7


def gelu_and_slope(h):
    root = 0.7978845608028654
    cube = 0.044715
    sq = h * h
    th = jnp.tanh(root * (h + cube * (h * sq)))
    cdf = 0.5 * (1.0 + th)
    slope = cdf + (0.5 * root) * h * (1.0 - th * th) * (1.0 + (3.0 * cube) * sq)
    return h * cdf, slope


def main_kernel(sizes, w_in, w_out, x_saved, h_saved, dy_in, acc_in, acc_out,
                m_ref, dx_ref,
                wi_s, wo_s, lt_s, rm_s, xs_s, cb_s, acc_s, p_s, h1_s, h2_s,
                wsem, hsem, xsem, dysem, accsem, cot_send, cot_recv, dx_send, dx_recv, dx_loc,
                send_sem, recv_sem, free_sem):
    hid, ff, tok, stages = sizes
    cw = hid // COLS
    nq = ff // cw
    nb = ff // hid
    per_kind = nq
    per_layer = 2 * nq
    total = 2 * per_layer
    unit = hid // 16
    tile = hid // TILES
    rows4 = stages * tok

    pp = lax.axis_index('pp')
    dp = lax.axis_index('dp')
    core = dp % 2
    xc = (dp // 2) % 2
    yc = dp // 4
    pair = dp + 1 - 2 * core
    xn = dp + 2 - 4 * xc
    yn = dp + 4 - 8 * yc

    def dev(pp_i, dp_i):
        return dict(device_id=(pp_i, dp_i), device_id_type=pl.DeviceIdType.MESH)

    def w_out_copy(k):
        return pltpu.make_async_copy(w_out.at[0, k], wo_s.at[k], wsem.at[k, 0])

    def w_in_start(k):
        for j in range(nb):
            pltpu.make_async_copy(w_in.at[0, k, :, pl.ds(j * hid, hid)], wi_s.at[k, j], wsem.at[k, 1]).start()

    def w_in_wait(k):
        pltpu.make_async_copy(wi_s.at[k], wi_s.at[k], wsem.at[k, 1]).wait()

    def h_start(part):
        def one(i, carry):
            k = 1 - i // nq
            q = i % nq
            pltpu.make_async_copy(h_saved.at[0, pl.ds(2 * part, 2), k, :, pl.ds(pl.multiple_of(q * cw, 128), cw)],
                                  rm_s.at[k, COLS + q, pl.ds(2 * part, 2)], hsem.at[part]).start()
            return carry
        lax.fori_loop(0, 2 * nq, one, 0)

    def h_wait(part):
        where = rm_s.at[:, pl.ds(COLS, nq), pl.ds(2 * part, 2)]
        pltpu.make_async_copy(where, where, hsem.at[part]).wait()

    def dy_start():
        for n in range(TILES):
            pltpu.make_async_copy(dy_in.at[0, :, pl.ds(n * tile, tile)], cb_s.at[0, n], dysem).start()

    def dy_wait():
        pltpu.make_async_copy(cb_s.at[0], cb_s.at[0], dysem).wait()

    x_copy = pltpu.make_async_copy(x_saved.at[0], xs_s, xsem)

    def acc_where(c):
        k = 1 - c // per_layer
        b = c % per_layer
        return k, b // per_kind, b % per_kind

    def acc_copies(c):
        k, kind, jj = acc_where(c)
        slot = c % 2
        a = pltpu.make_async_copy(acc_out.at[0, 0, k, pl.ds(pl.multiple_of((jj // COLS) * hid, 128), hid), pl.ds(pl.multiple_of((jj % COLS) * cw, 128), cw)],
                                  acc_s.at[slot], accsem.at[slot])
        b = pltpu.make_async_copy(acc_in.at[0, 0, k, :, pl.ds(pl.multiple_of(jj * cw, 128), cw)], acc_s.at[slot], accsem.at[slot])
        return kind, a, b

    def acc_start(c):
        kind, a, b = acc_copies(c)

        @pl.when(kind == 0)
        def _():
            a.start()

        @pl.when(kind == 1)
        def _():
            b.start()

    def acc_wait(c):
        acc_copies(c)[2].wait()

    dy_start()
    h_start(0)
    for k in (1, 0):
        w_out_copy(k).start()
        w_in_start(k)
    x_copy.start()
    for part in range(1, stages // 2):
        h_start(part)
    acc_start(0)

    barrier = pltpu.get_barrier_semaphore()
    for other in (pair, xn, yn):
        pl.semaphore_signal(barrier, inc=1, **dev(pp, other))
    for step in range(1, stages):
        pl.semaphore_signal(barrier, inc=1, **dev((pp + step) % stages, dp))

    def cot_copy(t, n):
        return pltpu.make_async_remote_copy(src_ref=cb_s.at[t, n], dst_ref=cb_s.at[t + 1, n], send_sem=cot_send.at[t, n], recv_sem=cot_recv.at[t + 1, n],
                                            **dev(jnp.maximum(pp - 1, 0), dp))

    def cot_arrival(t, n):
        return pltpu.make_async_remote_copy(src_ref=cb_s.at[t, n], dst_ref=cb_s.at[t, n], send_sem=cot_send.at[0, n], recv_sem=cot_recv.at[t, n],
                                            **dev(jnp.maximum(pp - 1, 0), dp))

    def dx_copy(t, n):
        return pltpu.make_async_remote_copy(src_ref=cb_s.at[t, n], dst_ref=dx_ref.at[0, :, pl.ds(n * tile, tile)], send_sem=dx_send.at[t, n], recv_sem=dx_recv.at[n],
                                            **dev(t, dp))

    def cot_now(t):
        return jnp.concatenate([cb_s[t, n] for n in range(TILES)], axis=1)

    def keep_cot(t, k, cot):
        for j in range(COLS):
            rm_s[k, j, t] = cot[:, j * cw:(j + 1) * cw]

    def layer(t, k, sends):
        cot = cot_now(t)
        keep_cot(t, k, cot)
        for j in range(nb):
            e = lax.dot_general(cot, wo_s[k, j * hid:(j + 1) * hid, :], NT, preferred_element_type=F32)
            for i in range(COLS):
                q = j * COLS + i
                _, slope = gelu_and_slope(rm_s[k, COLS + q, t].astype(F32))
                rm_s[k, COLS + q, t] = (e[:, i * cw:(i + 1) * cw] * slope).astype(BF16)
        for n in range(TILES):
            back = cot[:, n * tile:(n + 1) * tile].astype(F32)
            for j in range(nb):
                dh = jnp.concatenate([rm_s[k, COLS + j * COLS + i, t] for i in range(COLS)], axis=1)
                back += lax.dot_general(dh, wi_s[k, j, n * tile:(n + 1) * tile, :], NT, preferred_element_type=F32)
            cb_s[t, n] = back.astype(BF16)
            if sends:
                @pl.when(pp > 0)
                def _():
                    cot_copy(t, n).start()

                if not isinstance(t, int):
                    @pl.when(pp == 0)
                    def _():
                        dx_copy(t, n).start()

    def layers(t):
        layer(t, 1, False)
        layer(t, 0, True)

    def cot_wait(t):
        for n in range(TILES):
            cot_arrival(t, n).wait_recv()

    def prepare(k, carry):
        lt_s[k, 0] = jnp.concatenate([xs_s[t, k] for t in range(stages)], axis=0).T
        return carry

    def acts(part):
        def body(i, carry):
            k = 1 - i // nq
            q = i % nq
            hh = rm_s[k, COLS + q, 2 * part:2 * part + 2].reshape(2 * tok, cw).astype(F32)
            act, _ = gelu_and_slope(hh)
            lt_s[k, 1 + q // COLS, pl.ds(pl.multiple_of((q % COLS) * cw, 128), cw), 2 * part * tok:2 * (part + 1) * tok] = act.astype(BF16).T
            return carry
        lax.fori_loop(0, 2 * nq, body, 0)

    def zero_inactive(t, carry):
        zero = jnp.zeros((tok, cw), BF16)

        def one_layer(k, c2):
            for j in range(COLS + nq):
                rm_s[k, j, t] = zero
            return c2
        return lax.fori_loop(0, 2, one_layer, carry)

    last = stages - 1 - pp
    h_wait(0)
    acts(0)
    dy_wait()
    pl.semaphore_wait(barrier, 3 + stages - 1)
    w_out_copy(1).wait()
    w_in_wait(1)
    layer(0, 1, False)
    w_out_copy(0).wait()
    w_in_wait(0)
    layer(0, 0, True)
    x_copy.wait()
    lax.fori_loop(0, 2, prepare, 0)
    for part in range(1, stages // 2):
        h_wait(part)

    def middle(t, carry):
        cot_wait(t)
        layers(t)
        for part in range(1, stages // 2):
            @pl.when(t == 2 * part - 1)
            def _():
                acts(part)
        return carry

    lax.fori_loop(1, jnp.where(pp == 0, stages - 1, last + 1), middle, 0)

    @pl.when(last == 0)
    def _():
        for part in range(1, stages // 2):
            acts(part)
    lax.fori_loop(last + 1, stages, zero_inactive, 0)

    half = hid // 2
    hb = core * half
    xb = hb
    yb = hb + 4 * unit

    def rows_of(start, n):
        return pl.ds(pl.multiple_of(start, 16), n)

    def remote(kind, c, src, dst, target):
        return pltpu.make_async_remote_copy(src_ref=src, dst_ref=dst, send_sem=send_sem.at[kind, c % RING], recv_sem=recv_sem.at[kind, c % RECV_RING], **dev(pp, target))

    def msg(kind, c, arriving=False):
        f = 1 if arriving else 0
        if kind == 0:
            other = m_ref.at[c, rows_of(half - hb, half), :]
            return remote(0, c, other, p_s.at[c], pair)
        if kind == 1:
            return remote(1, c, p_s.at[c, rows_of((1 - xc) * 2 * unit, 2 * unit), :], h1_s.at[c, 0], xn)
        if kind == 2:
            return remote(2, c, p_s.at[c, rows_of(4 * unit + (1 - yc) * 2 * unit, 2 * unit), :], h1_s.at[c, 1], yn)
        if kind == 3:
            return remote(3, c, h1_s.at[c, 0, rows_of((1 - yc) * unit, unit), :], h2_s.at[c, 0], yn)
        if kind == 4:
            return remote(4, c, h1_s.at[c, 1, rows_of((1 - xc) * unit, unit), :], h2_s.at[c, 1], xn)
        if kind == 5:
            y_of = 1 - yc if f else yc
            r = m_ref.at[c, rows_of(xb + xc * 2 * unit + y_of * unit, unit), :]
            return remote(5, c, r, r, yn)
        if kind == 6:
            x_of = 1 - xc if f else xc
            r = m_ref.at[c, rows_of(yb + yc * 2 * unit + x_of * unit, unit), :]
            return remote(6, c, r, r, xn)
        if kind == 7:
            x_of = 1 - xc if f else xc
            r = m_ref.at[c, rows_of(xb + x_of * 2 * unit, 2 * unit), :]
            return remote(7, c, r, r, xn)
        if kind == 8:
            y_of = 1 - yc if f else yc
            r = m_ref.at[c, rows_of(yb + y_of * 2 * unit, 2 * unit), :]
            return remote(8, c, r, r, yn)
        base = half - hb if f else hb
        r = m_ref.at[c, rows_of(base, half), :]
        return remote(9, c, r, r, pair)

    def send(kind, c):
        if kind > 0:
            @pl.when(c >= RING)
            def _():
                msg(kind, c - RING).wait_send()
        msg(kind, c).start()

    def arrive(kind, c):
        msg(kind, c, True).wait_recv()

    def plus(left, right):
        return (left.astype(F32) + right.astype(F32)).astype(BF16)

    def produce(c):
        @pl.when(c + 1 < total)
        def _():
            acc_start(c + 1)
        acc_wait(c)
        k, kind, jj = acc_where(c)
        li = (1 - kind) * (1 + jj // COLS)
        ri = (1 - kind) * (jj % COLS) + kind * (COLS + jj)
        slot = c % 2
        right = rm_s[k, ri].reshape(rows4, cw)
        nr = hid // 6 if hid % 768 == 0 else hid // 2
        for i in range(hid // nr):
            r = pl.ds(i * nr, nr)
            g = jnp.dot(lt_s[k, li, r, :], right, preferred_element_type=F32)
            m_ref[c, r, :] = (acc_s[slot, r, :] + g).astype(BF16)
        send(0, c)

    def stage1(c):
        arrive(0, c)
        p_s[c] = plus(p_s[c], m_ref[c, rows_of(hb, half), :])
        send(1, c)
        send(2, c)
        msg(0, c).wait_send()
        pl.semaphore_signal(free_sem, inc=1, **dev(pp, pair))

    def stage2(c):
        arrive(1, c)
        h1_s[c, 0] = plus(h1_s[c, 0], p_s[c, rows_of(xc * 2 * unit, 2 * unit), :])
        send(3, c)
        arrive(2, c)
        h1_s[c, 1] = plus(h1_s[c, 1], p_s[c, rows_of(4 * unit + yc * 2 * unit, 2 * unit), :])
        send(4, c)

    def stage3(c):
        arrive(3, c)
        m_ref[c, rows_of(xb + xc * 2 * unit + yc * unit, unit), :] = plus(h1_s[c, 0, rows_of(yc * unit, unit), :], h2_s[c, 0])
        send(5, c)
        arrive(4, c)
        m_ref[c, rows_of(yb + yc * 2 * unit + xc * unit, unit), :] = plus(h1_s[c, 1, rows_of(xc * unit, unit), :], h2_s[c, 1])
        send(6, c)

    def stage4(c):
        arrive(5, c)
        send(7, c)
        arrive(6, c)
        send(8, c)

    def stage5(c):
        arrive(7, c)
        arrive(8, c)
        pl.semaphore_wait(free_sem, 1)
        send(9, c)

    def stage6(c):
        arrive(9, c)

    plan = ((stage6, 16), (stage5, 14), (stage4, 11), (stage3, 8), (stage2, 5), (stage1, 2), (produce, 0))
    depth = max(lag for _, lag in plan)

    def run(i, carry):
        for fn, lag in plan:
            c = i - lag

            @pl.when((c >= 0) & (c < total))
            def _():
                fn(c)
        return carry

    def finish(i, carry):
        @pl.when(i == EARLY)
        def _():
            @pl.when(pp == 0)
            def _():
                layers(jnp.int32(stages - 1))
        run(i, carry)
        return carry

    @pl.when(pp == 0)
    def _():
        cot_wait(stages - 1)
        keep_cot(stages - 1, 1, cot_now(stages - 1))
    lax.fori_loop(0, total + depth, finish, 0)

    def drain(i, carry):
        for kind in range(1, 10):
            msg(kind, total - RING + i).wait_send()
        return carry

    lax.fori_loop(0, RING, drain, 0)

    @pl.when(pp == 0)
    def _():
        for n in range(TILES):
            pltpu.make_async_copy(cb_s.at[0, n], dx_ref.at[0, :, pl.ds(n * tile, tile)], dx_loc).start()
        pltpu.make_async_copy(cb_s.at[0], cb_s.at[0], dx_loc).wait()

        def sent(t, carry):
            for n in range(TILES):
                dx_copy(t, n).wait_send()
            return carry
        lax.fori_loop(1, stages, sent, 0)

    @pl.when(pp > 0)
    def _():
        def sent(t, carry):
            for n in range(TILES):
                cot_copy(t, n).wait_send()
            return carry
        lax.fori_loop(0, stages - pp, sent, 0)
        for n in range(TILES):
            dx_copy(0, n).wait_recv()


def write_kernel(sizes, m_ref, gi_ref, go_ref, out_s, out_sem):
    hid, ff, tok, stages = sizes
    cw = hid // COLS
    nq = ff // cw
    per_layer = 2 * nq
    total = 2 * per_layer
    slots = out_s.shape[0]

    def copies(c):
        k = 1 - c // per_layer
        b = c % per_layer
        kind, jj = b // nq, b % nq
        slot = c % slots
        a = pltpu.make_async_copy(out_s.at[slot], go_ref.at[0, k, pl.ds(pl.multiple_of((jj // COLS) * hid, 128), hid), pl.ds(pl.multiple_of((jj % COLS) * cw, 128), cw)], out_sem.at[slot])
        b = pltpu.make_async_copy(out_s.at[slot], gi_ref.at[0, k, :, pl.ds(pl.multiple_of(jj * cw, 128), cw)], out_sem.at[slot])
        return kind, a, b

    def body(c, carry):
        @pl.when(c >= slots)
        def _():
            copies(c - slots)[2].wait()
        slot = c % slots
        nr = hid // 4
        for i in range(4):
            r = pl.ds(i * nr, nr)
            out_s[slot, r, :] = m_ref[c, r, :].astype(F32) * 0.125
        kind, a, b = copies(c)

        @pl.when(kind == 0)
        def _():
            a.start()

        @pl.when(kind == 1)
        def _():
            b.start()
        return carry

    lax.fori_loop(0, total, body, 0)

    def drain(i, carry):
        copies(total - slots + i)[2].wait()
        return carry
    lax.fori_loop(0, slots, drain, 0)


def solution(mesh):
    stages = mesh.shape['pp']

    def device_fn(w_in, w_out, x_saved, h_saved, dy_in, acc_in, acc_out):
        hid, ff = w_in.shape[2:]
        tok = dy_in.shape[1]
        sizes = (hid, ff, tok, stages)
        cw = hid // COLS
        nq = ff // cw
        total = 4 * nq
        unit = hid // 16
        any_spec = pl.BlockSpec(memory_space=pltpu.HBM)
        vm_spec = pl.BlockSpec(memory_space=pltpu.VMEM)
        m_all, dx = pl.pallas_call(
            functools.partial(main_kernel, sizes),
            out_shape=(pltpu.VMEM((total, hid, cw), BF16), jax.ShapeDtypeStruct((1, tok, hid), BF16)),
            in_specs=[any_spec] * 7,
            out_specs=(vm_spec, vm_spec),
            scratch_shapes=[
                pltpu.VMEM((2, ff // hid, hid, hid), BF16),
                pltpu.VMEM((2, ff, hid), BF16),
                pltpu.VMEM((2, 1 + ff // hid, hid, stages * tok), BF16),
                pltpu.VMEM((2, COLS + nq, stages, tok, cw), BF16),
                pltpu.VMEM((stages, 2, tok, hid), BF16),
                pltpu.VMEM((stages, TILES, tok, hid // TILES), BF16),
                pltpu.VMEM((2, hid, cw), F32),
                pltpu.VMEM((total, hid // 2, cw), BF16),
                pltpu.VMEM((total, 2, 2 * unit, cw), BF16),
                pltpu.VMEM((total, 2, unit, cw), BF16),
                pltpu.SemaphoreType.DMA((2, 2)),
                pltpu.SemaphoreType.DMA((stages // 2,)),
                pltpu.SemaphoreType.DMA,
                pltpu.SemaphoreType.DMA,
                pltpu.SemaphoreType.DMA((2,)),
                pltpu.SemaphoreType.DMA((stages, TILES)),
                pltpu.SemaphoreType.DMA((stages, TILES)),
                pltpu.SemaphoreType.DMA((stages, TILES)),
                pltpu.SemaphoreType.DMA((TILES,)),
                pltpu.SemaphoreType.DMA,
                pltpu.SemaphoreType.DMA((10, RING)),
                pltpu.SemaphoreType.DMA((10, RECV_RING)),
                pltpu.SemaphoreType.REGULAR,
            ],
            compiler_params=pltpu.CompilerParams(collective_id=0, has_side_effects=True, vmem_limit_bytes=46900 * 1024),
            name='chain_reduce',
        )(w_in, w_out, x_saved, h_saved, dy_in, acc_in, acc_out)
        grad_in, grad_out = pl.pallas_call(
            functools.partial(write_kernel, sizes),
            out_shape=(jax.ShapeDtypeStruct((1, 2, hid, ff), F32), jax.ShapeDtypeStruct((1, 2, ff, hid), F32)),
            in_specs=[vm_spec],
            out_specs=(any_spec, any_spec),
            scratch_shapes=[pltpu.VMEM((4, hid, cw), F32), pltpu.SemaphoreType.DMA((4,))],
            compiler_params=pltpu.CompilerParams(vmem_limit_bytes=16 * 1024 * 1024),
            name='write_out',
        )(m_all)
        return grad_in, grad_out, dx

    return jax.shard_map(device_fn, mesh=mesh, in_specs=(P('pp'), P('pp'), P('pp', None, None, 'dp'), P('pp', None, None, 'dp'), P('pp', 'dp'), P('pp', 'dp'), P('pp', 'dp')), out_specs=(P('pp'), P('pp'), P('pp', 'dp')), check_vma=False)
```

```python
import functools
import jax
import jax.numpy as jnp
from jax import lax
from jax.experimental import pallas as pl
from jax.experimental.pallas import tpu as pltpu
from jax.sharding import PartitionSpec as P

BF16 = jnp.bfloat16
F32 = jnp.float32
NT = (((1,), (1,)), ((), ()))
COLS = 2
TILES = 3
RING = 4
RECV_RING = 8
MOVED = (2, 1)
POS = 20
HAND = 9
EARLY = 7


def gelu_and_slope(h):
    root = 0.7978845608028654
    cube = 0.044715
    sq = h * h
    th = jnp.tanh(root * (h + cube * (h * sq)))
    cdf = 0.5 * (1.0 + th)
    slope = cdf + (0.5 * root) * h * (1.0 - th * th) * (1.0 + (3.0 * cube) * sq)
    return h * cdf, slope


def main_kernel(sizes, w_in, w_out, x_saved, h_saved, dy_in, acc_in, acc_out,
                m_ref, dx_ref,
                wi_s, wo_s, lt_s, rm_s, xs_s, cb_s, acc_s, p_s, h1_s, h2_s,
                wsem, hsem, xsem, dysem, accsem, cot_send, cot_recv,
                send_sem, recv_sem, free_sem, mv_send, mv_recv, z_free, mv_free):
    hid, ff, tok, stages = sizes
    cw = hid // COLS
    nq = ff // cw
    nb = ff // hid
    per_kind = nq
    per_layer = 2 * nq
    total = 2 * per_layer
    unit = hid // 16
    tile = hid // TILES
    rows4 = stages * tok

    pp = lax.axis_index('pp')
    dp = lax.axis_index('dp')
    core = dp % 2
    xc = (dp // 2) % 2
    yc = dp // 4
    pair = dp + 1 - 2 * core
    xn = dp + 2 - 4 * xc
    yn = dp + 4 - 8 * yc

    def dev(pp_i, dp_i):
        return dict(device_id=(pp_i, dp_i), device_id_type=pl.DeviceIdType.MESH)

    def w_out_copy(k):
        return pltpu.make_async_copy(w_out.at[0, k], wo_s.at[k], wsem.at[k, 0])

    def w_in_start(k):
        for j in range(nb):
            pltpu.make_async_copy(w_in.at[0, k, :, pl.ds(j * hid, hid)], wi_s.at[k, j], wsem.at[k, 1]).start()

    def w_in_wait(k):
        pltpu.make_async_copy(wi_s.at[k], wi_s.at[k], wsem.at[k, 1]).wait()

    def h_start(part):
        def one(i, carry):
            k = 1 - i // nq
            q = i % nq
            pltpu.make_async_copy(h_saved.at[0, pl.ds(2 * part, 2), k, :, pl.ds(pl.multiple_of(q * cw, 128), cw)],
                                  rm_s.at[k, COLS + q, pl.ds(2 * part, 2)], hsem.at[part]).start()
            return carry
        lax.fori_loop(0, 2 * nq, one, 0)

    def h_wait(part):
        where = rm_s.at[:, pl.ds(COLS, nq), pl.ds(2 * part, 2)]
        pltpu.make_async_copy(where, where, hsem.at[part]).wait()

    def dy_start():
        for n in range(TILES):
            pltpu.make_async_copy(dy_in.at[0, :, pl.ds(n * tile, tile)], cb_s.at[0, n], dysem).start()

    def dy_wait():
        pltpu.make_async_copy(cb_s.at[0], cb_s.at[0], dysem).wait()

    x_copy = pltpu.make_async_copy(x_saved.at[0], xs_s, xsem)

    def acc_where(c):
        k = 1 - c // per_layer
        b = c % per_layer
        return k, b // per_kind, b % per_kind

    def acc_copies(c, slot):
        k, kind, jj = acc_where(c)
        a = pltpu.make_async_copy(acc_out.at[0, 0, k, pl.ds(pl.multiple_of((jj // COLS) * hid, 128), hid), pl.ds(pl.multiple_of((jj % COLS) * cw, 128), cw)],
                                  acc_s.at[slot], accsem.at[slot])
        b = pltpu.make_async_copy(acc_in.at[0, 0, k, :, pl.ds(pl.multiple_of(jj * cw, 128), cw)], acc_s.at[slot], accsem.at[slot])
        return kind, a, b

    def acc_start(c, slot):
        kind, a, b = acc_copies(c, slot)

        @pl.when(kind == 0)
        def _():
            a.start()

        @pl.when(kind == 1)
        def _():
            b.start()

    def acc_wait(slot):
        pltpu.make_async_copy(acc_s.at[slot], acc_s.at[slot], accsem.at[slot]).wait()

    dy_start()
    h_start(0)
    for k in (1, 0):
        w_out_copy(k).start()
        w_in_start(k)
    x_copy.start()
    for part in range(1, stages // 2):
        h_start(part)
    acc_start(0, 0)

    barrier = pltpu.get_barrier_semaphore()
    for other in (pair, xn, yn):
        pl.semaphore_signal(barrier, inc=1, **dev(pp, other))
    for step in range(1, stages):
        pl.semaphore_signal(barrier, inc=1, **dev((pp + step) % stages, dp))

    def cot_copy(t, n):
        above = pp > 0
        spare = (stages - 1, stages - 2) if isinstance(t, int) else (t, stages - 1)
        slot = jnp.where(above, t + 1, spare[1])
        return pltpu.make_async_remote_copy(src_ref=cb_s.at[t, n], dst_ref=cb_s.at[slot, n], send_sem=cot_send.at[t, n], recv_sem=cot_recv.at[slot, n],
                                            **dev(jnp.where(above, pp - 1, spare[0]), dp))

    def cot_arrival(t, n):
        return pltpu.make_async_remote_copy(src_ref=cb_s.at[t, n], dst_ref=cb_s.at[t, n], send_sem=cot_send.at[0, n], recv_sem=cot_recv.at[t, n],
                                            **dev(jnp.maximum(pp - 1, 0), dp))

    def cot_now(t):
        return jnp.concatenate([cb_s[t, n] for n in range(TILES)], axis=1)

    def keep_cot(t, k, cot):
        for j in range(COLS):
            rm_s[k, j, t] = cot[:, j * cw:(j + 1) * cw]

    def layer(t, k, sends):
        cot = cot_now(t)
        keep_cot(t, k, cot)
        for j in range(nb):
            e = lax.dot_general(cot, wo_s[k, j * hid:(j + 1) * hid, :], NT, preferred_element_type=F32)
            for i in range(COLS):
                q = j * COLS + i
                _, slope = gelu_and_slope(rm_s[k, COLS + q, t].astype(F32))
                rm_s[k, COLS + q, t] = (e[:, i * cw:(i + 1) * cw] * slope).astype(BF16)
        for n in range(TILES):
            back = cot[:, n * tile:(n + 1) * tile].astype(F32)
            for j in range(nb):
                dh = jnp.concatenate([rm_s[k, COLS + j * COLS + i, t] for i in range(COLS)], axis=1)
                back += lax.dot_general(dh, wi_s[k, j, n * tile:(n + 1) * tile, :], NT, preferred_element_type=F32)
            cb_s[t, n] = back.astype(BF16)
            if sends:
                cot_copy(t, n).start()

    def layers(t):
        layer(t, 1, False)
        layer(t, 0, True)

    def cot_wait(t):
        for n in range(TILES):
            cot_arrival(t, n).wait_recv()

    def prepare(k, carry):
        lt_s[k, 0] = jnp.concatenate([xs_s[t, k] for t in range(stages)], axis=0).T
        return carry

    def acts(part):
        def body(i, carry):
            k = 1 - i // nq
            q = i % nq
            hh = rm_s[k, COLS + q, 2 * part:2 * part + 2].reshape(2 * tok, cw).astype(F32)
            act, _ = gelu_and_slope(hh)
            lt_s[k, 1 + q // COLS, pl.ds(pl.multiple_of((q % COLS) * cw, 128), cw), 2 * part * tok:2 * (part + 1) * tok] = act.astype(BF16).T
            return carry
        lax.fori_loop(0, 2 * nq, body, 0)

    def zero_inactive(t, carry):
        zero = jnp.zeros((tok, cw), BF16)

        def one_layer(k, c2):
            for j in range(COLS + nq):
                rm_s[k, j, t] = zero
            return c2
        return lax.fori_loop(0, 2, one_layer, carry)

    last = stages - 1 - pp
    h_wait(0)
    acts(0)
    dy_wait()
    pl.semaphore_wait(barrier, 3 + stages - 1)
    w_out_copy(1).wait()
    w_in_wait(1)
    layer(0, 1, False)
    w_out_copy(0).wait()
    w_in_wait(0)
    layer(0, 0, True)
    x_copy.wait()
    lax.fori_loop(0, 2, prepare, 0)
    for part in range(1, stages // 2):
        h_wait(part)

    def middle(t, carry):
        cot_wait(t)
        layers(t)
        for part in range(1, stages // 2):
            @pl.when(t == 2 * part - 1)
            def _():
                acts(part)
        return carry

    lax.fori_loop(1, jnp.where(pp == 0, stages - 1, last + 1), middle, 0)

    @pl.when(last == 0)
    def _():
        for part in range(1, stages // 2):
            acts(part)
    lax.fori_loop(last + 1, stages, zero_inactive, 0)

    half = hid // 2
    hb = core * half
    xb = hb
    yb = hb + 4 * unit
    zp = stages - 1 - pp
    helper = pp >= stages // 2
    moved = jnp.where((pp == 0) | (pp == stages - 1), MOVED[0], MOVED[1])
    steps = jnp.where(helper, total + moved, total - moved)
    own = jnp.where(helper, total, total - moved)

    def is_foreign(i):
        return helper & (i >= POS) & (i < POS + moved)

    def own_of(i):
        return jnp.where(helper & (i >= POS), i - moved, i)

    def rows_of(start, n):
        return pl.ds(pl.multiple_of(start, 16), n)

    def msg(kind, i, foreign, arriving=False):
        f = 1 if arriving else 0
        c = i - POS if foreign else own_of(i)

        def remote(src, dst, target):
            j = c if kind in (0, 9) else i
            return pltpu.make_async_remote_copy(src_ref=src, dst_ref=dst, send_sem=send_sem.at[kind, j % RING], recv_sem=recv_sem.at[kind, j % RECV_RING], **dev(pp, target))

        def place(start, n):
            return p_s.at[c, rows_of(start, n), :] if foreign else m_ref.at[c, rows_of(hb + start, n), :]
        yp = 4 * unit
        if kind == 0:
            return remote(m_ref.at[c, rows_of(half - hb, half), :], p_s.at[c], pair)
        if kind == 1:
            return remote(p_s.at[c, rows_of((1 - xc) * 2 * unit, 2 * unit), :], h1_s.at[c, 0], xn)
        if kind == 2:
            return remote(p_s.at[c, rows_of(yp + (1 - yc) * 2 * unit, 2 * unit), :], h1_s.at[c, 1], yn)
        if kind == 3:
            return remote(h1_s.at[c, 0, rows_of((1 - yc) * unit, unit), :], h2_s.at[c, 0], yn)
        if kind == 4:
            return remote(h1_s.at[c, 1, rows_of((1 - xc) * unit, unit), :], h2_s.at[c, 1], xn)
        if kind == 5:
            y_of = 1 - yc if f else yc
            r = place(xc * 2 * unit + y_of * unit, unit)
            return remote(r, r, yn)
        if kind == 6:
            x_of = 1 - xc if f else xc
            r = place(yp + yc * 2 * unit + x_of * unit, unit)
            return remote(r, r, xn)
        if kind == 7:
            x_of = 1 - xc if f else xc
            r = place(x_of * 2 * unit, 2 * unit)
            return remote(r, r, xn)
        if kind == 8:
            y_of = 1 - yc if f else yc
            r = place(yp + y_of * 2 * unit, 2 * unit)
            return remote(r, r, yn)
        r = m_ref.at[c, rows_of(half - hb if f else hb, half), :]
        return remote(r, r, pair)

    def moved_msg(kind, f, arriving=False):
        c = total - moved + f

        def remote(src, dst, pp_i, dp_i):
            return pltpu.make_async_remote_copy(src_ref=src, dst_ref=dst, send_sem=mv_send.at[kind, f], recv_sem=mv_recv.at[kind, f], **dev(pp_i, dp_i))
        if kind == 0:
            return remote(m_ref.at[c, rows_of(half - hb, half), :], p_s.at[c], pp, pair)
        if kind == 1:
            return remote(p_s.at[c], p_s.at[f], zp, dp)
        if kind == 2:
            return remote(p_s.at[f], m_ref.at[c, rows_of(hb, half), :], zp, dp)
        r = m_ref.at[c, rows_of(half - hb if arriving else hb, half), :]
        return remote(r, r, pp, pair)

    def send(kind, i, foreign):
        if kind >= 3:
            j = own_of(i) if kind == 9 else i

            @pl.when(j >= RING)
            def _():
                wait_sent(kind, i)
        msg(kind, i, foreign).start()

    def wait_sent(kind, i):
        msg(kind, i, False).wait_send()

    def arrive(kind, i, foreign):
        msg(kind, i, foreign, True).wait_recv()

    def plus(left, right):
        return (left.astype(F32) + right.astype(F32)).astype(BF16)

    def product(c, slot):
        k, kind, jj = acc_where(c)
        li = (1 - kind) * (1 + jj // COLS)
        ri = (1 - kind) * (jj % COLS) + kind * (COLS + jj)
        right = rm_s[k, ri].reshape(rows4, cw)
        nr = hid // 6 if hid % 768 == 0 else hid // 2
        for n in range(hid // nr):
            r = pl.ds(n * nr, nr)
            g = jnp.dot(lt_s[k, li, r, :], right, preferred_element_type=F32)
            m_ref[c, r, :] = (acc_s[slot, r, :] + g).astype(BF16)

    def produce(i, foreign):
        if foreign:
            return
        c = own_of(i)

        @pl.when(c + 1 < own)
        def _():
            acc_start(c + 1, (c + 1) % 2)
        acc_wait(c % 2)
        product(c, c % 2)
        send(0, i, False)

    def stage1(i, foreign):
        if foreign:
            f = i - POS
            moved_msg(1, f, True).wait_recv()
            send(1, i, True)
            send(2, i, True)
            return
        c = own_of(i)
        arrive(0, i, False)
        p_s[c] = plus(p_s[c], m_ref[c, rows_of(hb, half), :])
        send(1, i, False)
        send(2, i, False)
        wait_sent(0, i)
        pl.semaphore_signal(free_sem, inc=1, **dev(pp, pair))

    def stage2(i, foreign):
        c = i - POS if foreign else own_of(i)
        arrive(1, i, foreign)
        h1_s[c, 0] = plus(h1_s[c, 0], p_s[c, rows_of(xc * 2 * unit, 2 * unit), :])
        wait_sent(2, i)
        send(3, i, foreign)
        arrive(2, i, foreign)
        h1_s[c, 1] = plus(h1_s[c, 1], p_s[c, rows_of(4 * unit + yc * 2 * unit, 2 * unit), :])
        wait_sent(1, i)
        send(4, i, foreign)
        if not foreign:
            @pl.when(helper & (i < moved))
            def _():
                pl.semaphore_signal(z_free, inc=1, **dev(zp, dp))

    def stage3(i, foreign):
        c = i - POS if foreign else own_of(i)

        def keep(start, value):
            if foreign:
                p_s[c, rows_of(start, unit), :] = value
            else:
                m_ref[c, rows_of(hb + start, unit), :] = value
        arrive(3, i, foreign)
        keep(xc * 2 * unit + yc * unit, plus(h1_s[c, 0, rows_of(yc * unit, unit), :], h2_s[c, 0]))
        send(5, i, foreign)
        arrive(4, i, foreign)
        keep(4 * unit + yc * 2 * unit + xc * unit, plus(h1_s[c, 1, rows_of(xc * unit, unit), :], h2_s[c, 1]))
        send(6, i, foreign)

    def stage4(i, foreign):
        arrive(5, i, foreign)
        send(7, i, foreign)
        arrive(6, i, foreign)
        send(8, i, foreign)

    def stage5(i, foreign):
        arrive(7, i, foreign)
        arrive(8, i, foreign)
        if foreign:
            moved_msg(2, i - POS).start()
            return
        pl.semaphore_wait(free_sem, 1)
        send(9, i, False)

    def stage6(i, foreign):
        if not foreign:
            arrive(9, i, False)

    plan = ((stage6, 16), (stage5, 14), (stage4, 11), (stage3, 8), (stage2, 5), (stage1, 2), (produce, 0))
    depth = max(lag for _, lag in plan)

    def run(i):
        for fn, lag in plan:
            j = i - lag
            live = (j >= 0) & (j < steps)

            @pl.when(live & jnp.logical_not(is_foreign(j)))
            def _():
                fn(j, False)

            if fn not in (produce, stage6):
                @pl.when(live & is_foreign(j))
                def _():
                    fn(j, True)

    def hand_over(i):
        @pl.when((i >= HAND) & (i < HAND + moved))
        def _():
            f = i - HAND
            c = total - moved + f
            acc_start(c, i % 2)
            acc_wait(i % 2)
            product(c, i % 2)
            moved_msg(0, f).start()

        @pl.when((i >= HAND + 2) & (i < HAND + 2 + moved))
        def _():
            f = i - HAND - 2
            c = total - moved + f
            moved_msg(0, f).wait_recv()
            p_s[c] = plus(p_s[c], m_ref[c, rows_of(hb, half), :])
            moved_msg(0, f).wait_send()
            pl.semaphore_signal(mv_free, inc=1, **dev(pp, pair))
            pl.semaphore_wait(z_free, 1)
            moved_msg(1, f).start()

    def step(i, carry):
        @pl.when(pp == 0)
        def _():
            @pl.when(i == EARLY)
            def _():
                layers(jnp.int32(stages - 1))
        run(i)

        @pl.when(jnp.logical_not(helper))
        def _():
            hand_over(i)
        return carry

    @pl.when(pp == 0)
    def _():
        cot_wait(stages - 1)
        keep_cot(stages - 1, 1, cot_now(stages - 1))
    lax.fori_loop(0, steps + depth, step, 0)

    @pl.when(jnp.logical_not(helper))
    def _():
        def give(f, carry):
            moved_msg(2, f).wait_recv()
            pl.semaphore_wait(mv_free, 1)
            moved_msg(3, f).start()
            return carry
        lax.fori_loop(0, moved, give, 0)

        def take(f, carry):
            moved_msg(3, f, True).wait_recv()
            moved_msg(3, f).wait_send()
            moved_msg(1, f).wait_send()
            return carry
        lax.fori_loop(0, moved, take, 0)

    @pl.when(helper)
    def _():
        def back(f, carry):
            moved_msg(2, f).wait_send()
            return carry
        lax.fori_loop(0, moved, back, 0)

    def drain(i, carry):
        for kind in range(3, 10):
            msg(kind, steps - RING + i, False).wait_send()
        return carry

    lax.fori_loop(0, RING, drain, 0)

    @pl.when(pp > 0)
    def _():
        cot_wait(stages - 1)

    @pl.when(pp == stages - 1)
    def _():
        cot_wait(stages - 2)

    def sent(t, carry):
        for n in range(TILES):
            cot_copy(t, n).wait_send()
        return carry
    lax.fori_loop(0, stages - pp, sent, 0)
    out_slot = jnp.where(pp == 0, 0, stages - 1)
    for n in range(TILES):
        dx_ref[0, :, n * tile:(n + 1) * tile] = cb_s[out_slot, n]


def write_kernel(sizes, m_ref, gi_ref, go_ref, out_s, out_sem):
    hid, ff, tok, stages = sizes
    cw = hid // COLS
    nq = ff // cw
    per_layer = 2 * nq
    total = 2 * per_layer
    slots = out_s.shape[0]

    def copies(c):
        k = 1 - c // per_layer
        b = c % per_layer
        kind, jj = b // nq, b % nq
        slot = c % slots
        a = pltpu.make_async_copy(out_s.at[slot], go_ref.at[0, k, pl.ds(pl.multiple_of((jj // COLS) * hid, 128), hid), pl.ds(pl.multiple_of((jj % COLS) * cw, 128), cw)], out_sem.at[slot])
        b = pltpu.make_async_copy(out_s.at[slot], gi_ref.at[0, k, :, pl.ds(pl.multiple_of(jj * cw, 128), cw)], out_sem.at[slot])
        return kind, a, b

    def body(c, carry):
        @pl.when(c >= slots)
        def _():
            copies(c - slots)[2].wait()
        slot = c % slots
        nr = hid // 4
        for i in range(4):
            r = pl.ds(i * nr, nr)
            out_s[slot, r, :] = m_ref[c, r, :].astype(F32) * 0.125
        kind, a, b = copies(c)

        @pl.when(kind == 0)
        def _():
            a.start()

        @pl.when(kind == 1)
        def _():
            b.start()
        return carry

    lax.fori_loop(0, total, body, 0)

    def drain(i, carry):
        copies(total - slots + i)[2].wait()
        return carry
    lax.fori_loop(0, slots, drain, 0)


def solution(mesh):
    stages = mesh.shape['pp']

    def device_fn(w_in, w_out, x_saved, h_saved, dy_in, acc_in, acc_out):
        hid, ff = w_in.shape[2:]
        tok = dy_in.shape[1]
        sizes = (hid, ff, tok, stages)
        cw = hid // COLS
        nq = ff // cw
        total = 4 * nq
        unit = hid // 16
        any_spec = pl.BlockSpec(memory_space=pltpu.HBM)
        vm_spec = pl.BlockSpec(memory_space=pltpu.VMEM)
        m_all, dx = pl.pallas_call(
            functools.partial(main_kernel, sizes),
            out_shape=(pltpu.VMEM((total, hid, cw), BF16), jax.ShapeDtypeStruct((1, tok, hid), BF16)),
            in_specs=[any_spec] * 7,
            out_specs=(vm_spec, vm_spec),
            scratch_shapes=[
                pltpu.VMEM((2, ff // hid, hid, hid), BF16),
                pltpu.VMEM((2, ff, hid), BF16),
                pltpu.VMEM((2, 1 + ff // hid, hid, stages * tok), BF16),
                pltpu.VMEM((2, COLS + nq, stages, tok, cw), BF16),
                pltpu.VMEM((stages, 2, tok, hid), BF16),
                pltpu.VMEM((stages, TILES, tok, hid // TILES), BF16),
                pltpu.VMEM((2, hid, cw), F32),
                pltpu.VMEM((total, hid // 2, cw), BF16),
                pltpu.VMEM((total, 2, 2 * unit, cw), BF16),
                pltpu.VMEM((total, 2, unit, cw), BF16),
                pltpu.SemaphoreType.DMA((2, 2)),
                pltpu.SemaphoreType.DMA((stages // 2,)),
                pltpu.SemaphoreType.DMA,
                pltpu.SemaphoreType.DMA,
                pltpu.SemaphoreType.DMA((2,)),
                pltpu.SemaphoreType.DMA((stages, TILES)),
                pltpu.SemaphoreType.DMA((stages, TILES)),
                pltpu.SemaphoreType.DMA((10, RING)),
                pltpu.SemaphoreType.DMA((10, RECV_RING)),
                pltpu.SemaphoreType.REGULAR,
                pltpu.SemaphoreType.DMA((4, max(MOVED))),
                pltpu.SemaphoreType.DMA((4, max(MOVED))),
                pltpu.SemaphoreType.REGULAR,
                pltpu.SemaphoreType.REGULAR,
            ],
            compiler_params=pltpu.CompilerParams(collective_id=0, has_side_effects=True, vmem_limit_bytes=46900 * 1024),
            name='chain_reduce',
        )(w_in, w_out, x_saved, h_saved, dy_in, acc_in, acc_out)
        grad_in, grad_out = pl.pallas_call(
            functools.partial(write_kernel, sizes),
            out_shape=(jax.ShapeDtypeStruct((1, 2, hid, ff), F32), jax.ShapeDtypeStruct((1, 2, ff, hid), F32)),
            in_specs=[vm_spec],
            out_specs=(any_spec, any_spec),
            scratch_shapes=[pltpu.VMEM((4, hid, cw), F32), pltpu.SemaphoreType.DMA((4,))],
            compiler_params=pltpu.CompilerParams(vmem_limit_bytes=16 * 1024 * 1024),
            name='write_out',
        )(m_all)
        return grad_in, grad_out, dx

    return jax.shard_map(device_fn, mesh=mesh, in_specs=(P('pp'), P('pp'), P('pp', None, None, 'dp'), P('pp', None, None, 'dp'), P('pp', 'dp'), P('pp', 'dp'), P('pp', 'dp')), out_specs=(P('pp'), P('pp'), P('pp', 'dp')), check_vma=False)
```

```python
import functools
import jax
import jax.numpy as jnp
from jax import lax
from jax.experimental import pallas as pl
from jax.experimental.pallas import tpu as pltpu
from jax.sharding import PartitionSpec as P

BF16 = jnp.bfloat16
F32 = jnp.float32
NT = (((1,), (1,)), ((), ()))
COLS = 3
TILES = 3
RING = 4
RECV_RING = 8
MOVED = (4, 1)
POS = 26
HAND = 13
EARLY = 10


def gelu_and_slope(h):
    root = 0.7978845608028654
    cube = 0.044715
    sq = h * h
    th = jnp.tanh(root * (h + cube * (h * sq)))
    cdf = 0.5 * (1.0 + th)
    slope = cdf + (0.5 * root) * h * (1.0 - th * th) * (1.0 + (3.0 * cube) * sq)
    return h * cdf, slope


def main_kernel(sizes, w_in, w_out, x_saved, h_saved, dy_in, acc_in, acc_out,
                m_ref, dx_ref,
                wi_s, wo_s, lt_s, rm_s, xs_s, cb_s, acc_s, p_s, h1_s, h2_s,
                wsem, hsem, xsem, dysem, accsem, cot_send, cot_recv,
                send_sem, recv_sem, free_sem, mv_send, mv_recv, z_free, mv_free):
    hid, ff, tok, stages = sizes
    cw = hid // COLS
    nq = ff // cw
    nb = ff // hid
    per_kind = nq
    per_layer = 2 * nq
    total = 2 * per_layer
    unit = hid // 16
    tile = hid // TILES
    rows4 = stages * tok

    pp = lax.axis_index('pp')
    dp = lax.axis_index('dp')
    core = dp % 2
    xc = (dp // 2) % 2
    yc = dp // 4
    pair = dp + 1 - 2 * core
    xn = dp + 2 - 4 * xc
    yn = dp + 4 - 8 * yc

    def dev(pp_i, dp_i):
        return dict(device_id=(pp_i, dp_i), device_id_type=pl.DeviceIdType.MESH)

    def w_out_copy(k):
        return pltpu.make_async_copy(w_out.at[0, k], wo_s.at[k], wsem.at[k, 0])

    def w_in_start(k):
        for j in range(nb):
            pltpu.make_async_copy(w_in.at[0, k, :, pl.ds(j * hid, hid)], wi_s.at[k, j], wsem.at[k, 1]).start()

    def w_in_wait(k):
        pltpu.make_async_copy(wi_s.at[k], wi_s.at[k], wsem.at[k, 1]).wait()

    def h_start(part):
        def one(i, carry):
            k = 1 - i // nq
            q = i % nq
            pltpu.make_async_copy(h_saved.at[0, pl.ds(2 * part, 2), k, :, pl.ds(pl.multiple_of(q * cw, 128), cw)],
                                  rm_s.at[k, COLS + q, pl.ds(2 * part, 2)], hsem.at[part]).start()
            return carry
        lax.fori_loop(0, 2 * nq, one, 0)

    def h_wait(part):
        where = rm_s.at[:, pl.ds(COLS, nq), pl.ds(2 * part, 2)]
        pltpu.make_async_copy(where, where, hsem.at[part]).wait()

    def dy_start():
        for n in range(TILES):
            pltpu.make_async_copy(dy_in.at[0, :, pl.ds(n * tile, tile)], cb_s.at[0, n], dysem).start()

    def dy_wait():
        pltpu.make_async_copy(cb_s.at[0], cb_s.at[0], dysem).wait()

    x_copy = pltpu.make_async_copy(x_saved.at[0], xs_s, xsem)

    def acc_where(c):
        k = 1 - c // per_layer
        b = c % per_layer
        return k, b // per_kind, b % per_kind

    def acc_copies(c, slot):
        k, kind, jj = acc_where(c)
        a = pltpu.make_async_copy(acc_out.at[0, 0, k, pl.ds(pl.multiple_of((jj // COLS) * hid, 128), hid), pl.ds(pl.multiple_of((jj % COLS) * cw, 128), cw)],
                                  acc_s.at[slot], accsem.at[slot])
        b = pltpu.make_async_copy(acc_in.at[0, 0, k, :, pl.ds(pl.multiple_of(jj * cw, 128), cw)], acc_s.at[slot], accsem.at[slot])
        return kind, a, b

    def acc_start(c, slot):
        kind, a, b = acc_copies(c, slot)

        @pl.when(kind == 0)
        def _():
            a.start()

        @pl.when(kind == 1)
        def _():
            b.start()

    def acc_wait(slot):
        pltpu.make_async_copy(acc_s.at[slot], acc_s.at[slot], accsem.at[slot]).wait()

    dy_start()
    h_start(0)
    w_out_copy(1).start()
    w_in_start(1)

    barrier = pltpu.get_barrier_semaphore()
    for other in (pair, xn, yn):
        pl.semaphore_signal(barrier, inc=1, **dev(pp, other))
    for step in range(1, stages):
        pl.semaphore_signal(barrier, inc=1, **dev((pp + step) % stages, dp))

    def cot_copy(t, n):
        above = pp > 0
        spare = (stages - 1, stages - 2) if isinstance(t, int) else (t, stages - 1)
        slot = jnp.where(above, t + 1, spare[1])
        return pltpu.make_async_remote_copy(src_ref=cb_s.at[t, n], dst_ref=cb_s.at[slot, n], send_sem=cot_send.at[t, n], recv_sem=cot_recv.at[slot, n],
                                            **dev(jnp.where(above, pp - 1, spare[0]), dp))

    def cot_arrival(t, n):
        return pltpu.make_async_remote_copy(src_ref=cb_s.at[t, n], dst_ref=cb_s.at[t, n], send_sem=cot_send.at[0, n], recv_sem=cot_recv.at[t, n],
                                            **dev(jnp.maximum(pp - 1, 0), dp))

    def cot_now(t):
        return jnp.concatenate([cb_s[t, n] for n in range(TILES)], axis=1)

    def keep_cot(t, k, cot):
        for j in range(COLS):
            rm_s[k, j, t] = cot[:, j * cw:(j + 1) * cw]

    def layer(t, k, sends):
        cot = cot_now(t)
        keep_cot(t, k, cot)
        for j in range(nb):
            e = lax.dot_general(cot, wo_s[k, j * hid:(j + 1) * hid, :], NT, preferred_element_type=F32)
            for i in range(COLS):
                q = j * COLS + i
                _, slope = gelu_and_slope(rm_s[k, COLS + q, t].astype(F32))
                rm_s[k, COLS + q, t] = (e[:, i * cw:(i + 1) * cw] * slope).astype(BF16)
        for n in range(TILES):
            back = cot[:, n * tile:(n + 1) * tile].astype(F32)
            for j in range(nb):
                dh = jnp.concatenate([rm_s[k, COLS + j * COLS + i, t] for i in range(COLS)], axis=1)
                back += lax.dot_general(dh, wi_s[k, j, n * tile:(n + 1) * tile, :], NT, preferred_element_type=F32)
            cb_s[t, n] = back.astype(BF16)
            if sends:
                cot_copy(t, n).start()

    def layers(t):
        layer(t, 1, False)
        layer(t, 0, True)

    def cot_wait(t):
        for n in range(TILES):
            cot_arrival(t, n).wait_recv()

    def prepare(k, carry):
        lt_s[k, 0] = jnp.concatenate([xs_s[t, k] for t in range(stages)], axis=0).T
        return carry

    def acts(part):
        def body(i, carry):
            k = 1 - i // nq
            q = i % nq
            hh = rm_s[k, COLS + q, 2 * part:2 * part + 2].reshape(2 * tok, cw).astype(F32)
            act, _ = gelu_and_slope(hh)
            lt_s[k, 1 + q // COLS, pl.ds(pl.multiple_of((q % COLS) * cw, 128), cw), 2 * part * tok:2 * (part + 1) * tok] = act.astype(BF16).T
            return carry
        lax.fori_loop(0, 2 * nq, body, 0)

    def zero_inactive(t, carry):
        zero = jnp.zeros((tok, cw), BF16)

        def one_layer(k, c2):
            for j in range(COLS + nq):
                rm_s[k, j, t] = zero
            return c2
        return lax.fori_loop(0, 2, one_layer, carry)

    last = stages - 1 - pp
    h_wait(0)
    w_out_copy(0).start()
    w_in_start(0)
    acts(0)
    dy_wait()
    pl.semaphore_wait(barrier, 3 + stages - 1)
    w_out_copy(1).wait()
    w_in_wait(1)
    layer(0, 1, False)
    x_copy.start()
    w_out_copy(0).wait()
    w_in_wait(0)
    layer(0, 0, True)
    acc_start(0, 0)
    for part in range(1, stages // 2):
        h_start(part)
    x_copy.wait()
    lax.fori_loop(0, 2, prepare, 0)
    for part in range(1, stages // 2):
        h_wait(part)

    def middle(t, carry):
        cot_wait(t)
        layers(t)
        for part in range(1, stages // 2):
            @pl.when(t == 2 * part - 1)
            def _():
                acts(part)
        return carry

    lax.fori_loop(1, jnp.where(pp == 0, stages - 1, last + 1), middle, 0)

    @pl.when(last == 0)
    def _():
        def blank(i, carry):
            lt_s[1 - i // (1 + nb), i % (1 + nb), :, 2 * tok:] = jnp.zeros((hid, (stages - 2) * tok), BF16)
            return carry
        lax.fori_loop(0, 2 * (1 + nb), blank, 0)
    lax.fori_loop(last + 1, stages, zero_inactive, 0)

    half = hid // 2
    hb = core * half
    xb = hb
    yb = hb + 4 * unit
    zp = stages - 1 - pp
    helper = pp >= stages // 2
    moved = jnp.where((pp == 0) | (pp == stages - 1), MOVED[0], MOVED[1])
    steps = jnp.where(helper, total + moved, total - moved)
    own = jnp.where(helper, total, total - moved)

    def is_foreign(i):
        return helper & (i >= POS) & (i < POS + moved)

    def own_of(i):
        return jnp.where(helper & (i >= POS), i - moved, i)

    def rows_of(start, n):
        return pl.ds(pl.multiple_of(start, 16), n)

    def msg(kind, i, foreign, arriving=False):
        f = 1 if arriving else 0
        c = i - POS if foreign else own_of(i)

        def remote(src, dst, target):
            j = c if kind in (0, 9) else i
            return pltpu.make_async_remote_copy(src_ref=src, dst_ref=dst, send_sem=send_sem.at[kind, j % RING], recv_sem=recv_sem.at[kind, j % RECV_RING], **dev(pp, target))

        def place(start, n):
            return p_s.at[c, rows_of(start, n), :] if foreign else m_ref.at[c, rows_of(hb + start, n), :]
        yp = 4 * unit
        if kind == 0:
            return remote(m_ref.at[c, rows_of(half - hb, half), :], p_s.at[c], pair)
        if kind == 1:
            return remote(p_s.at[c, rows_of((1 - xc) * 2 * unit, 2 * unit), :], h1_s.at[c, 0], xn)
        if kind == 2:
            return remote(p_s.at[c, rows_of(yp + (1 - yc) * 2 * unit, 2 * unit), :], h1_s.at[c, 1], yn)
        if kind == 3:
            return remote(h1_s.at[c, 0, rows_of((1 - yc) * unit, unit), :], h2_s.at[c, 0], yn)
        if kind == 4:
            return remote(h1_s.at[c, 1, rows_of((1 - xc) * unit, unit), :], h2_s.at[c, 1], xn)
        if kind == 5:
            y_of = 1 - yc if f else yc
            r = place(xc * 2 * unit + y_of * unit, unit)
            return remote(r, r, yn)
        if kind == 6:
            x_of = 1 - xc if f else xc
            r = place(yp + yc * 2 * unit + x_of * unit, unit)
            return remote(r, r, xn)
        if kind == 7:
            x_of = 1 - xc if f else xc
            r = place(x_of * 2 * unit, 2 * unit)
            return remote(r, r, xn)
        if kind == 8:
            y_of = 1 - yc if f else yc
            r = place(yp + y_of * 2 * unit, 2 * unit)
            return remote(r, r, yn)
        r = m_ref.at[c, rows_of(half - hb if f else hb, half), :]
        return remote(r, r, pair)

    def moved_msg(kind, f, arriving=False):
        c = total - moved + f

        def remote(src, dst, pp_i, dp_i):
            return pltpu.make_async_remote_copy(src_ref=src, dst_ref=dst, send_sem=mv_send.at[kind, f], recv_sem=mv_recv.at[kind, f], **dev(pp_i, dp_i))
        if kind == 0:
            return remote(m_ref.at[c, rows_of(half - hb, half), :], p_s.at[c], pp, pair)
        if kind == 1:
            return remote(p_s.at[c], p_s.at[f], zp, dp)
        if kind == 2:
            return remote(p_s.at[f], m_ref.at[c, rows_of(hb, half), :], zp, dp)
        r = m_ref.at[c, rows_of(half - hb if arriving else hb, half), :]
        return remote(r, r, pp, pair)

    def send(kind, i, foreign):
        if kind >= 3:
            j = own_of(i) if kind == 9 else i

            @pl.when(j >= RING)
            def _():
                wait_sent(kind, i)
        msg(kind, i, foreign).start()

    def wait_sent(kind, i):
        msg(kind, i, False).wait_send()

    def arrive(kind, i, foreign):
        msg(kind, i, foreign, True).wait_recv()

    def plus(left, right):
        return (left.astype(F32) + right.astype(F32)).astype(BF16)

    def product(c, slot):
        k, kind, jj = acc_where(c)
        li = (1 - kind) * (1 + jj // COLS)
        ri = (1 - kind) * (jj % COLS) + kind * (COLS + jj)
        right = rm_s[k, ri].reshape(rows4, cw)
        nr = hid // 6 if hid % 768 == 0 else hid // 2
        for n in range(hid // nr):
            r = pl.ds(n * nr, nr)
            g = jnp.dot(lt_s[k, li, r, :], right, preferred_element_type=F32)
            m_ref[c, r, :] = (acc_s[slot, r, :] + g).astype(BF16)

    def produce(i, foreign):
        if foreign:
            return
        c = own_of(i)

        @pl.when(c + 1 < own)
        def _():
            acc_start(c + 1, (c + 1) % 2)
        acc_wait(c % 2)
        product(c, c % 2)
        send(0, i, False)

    def stage1(i, foreign):
        if foreign:
            f = i - POS
            moved_msg(1, f, True).wait_recv()
            send(1, i, True)
            send(2, i, True)
            return
        c = own_of(i)
        arrive(0, i, False)
        p_s[c] = plus(p_s[c], m_ref[c, rows_of(hb, half), :])
        send(1, i, False)
        send(2, i, False)
        wait_sent(0, i)
        pl.semaphore_signal(free_sem, inc=1, **dev(pp, pair))

    def stage2(i, foreign):
        c = i - POS if foreign else own_of(i)
        arrive(1, i, foreign)
        h1_s[c, 0] = plus(h1_s[c, 0], p_s[c, rows_of(xc * 2 * unit, 2 * unit), :])
        wait_sent(2, i)
        send(3, i, foreign)
        arrive(2, i, foreign)
        h1_s[c, 1] = plus(h1_s[c, 1], p_s[c, rows_of(4 * unit + yc * 2 * unit, 2 * unit), :])
        wait_sent(1, i)
        send(4, i, foreign)
        if not foreign:
            @pl.when(helper & (i < moved))
            def _():
                pl.semaphore_signal(z_free, inc=1, **dev(zp, dp))

    def stage3(i, foreign):
        c = i - POS if foreign else own_of(i)

        def keep(start, value):
            if foreign:
                p_s[c, rows_of(start, unit), :] = value
            else:
                m_ref[c, rows_of(hb + start, unit), :] = value
        arrive(3, i, foreign)
        keep(xc * 2 * unit + yc * unit, plus(h1_s[c, 0, rows_of(yc * unit, unit), :], h2_s[c, 0]))
        send(5, i, foreign)
        arrive(4, i, foreign)
        keep(4 * unit + yc * 2 * unit + xc * unit, plus(h1_s[c, 1, rows_of(xc * unit, unit), :], h2_s[c, 1]))
        send(6, i, foreign)

    def stage4(i, foreign):
        arrive(5, i, foreign)
        send(7, i, foreign)
        arrive(6, i, foreign)
        send(8, i, foreign)

    def stage5(i, foreign):
        arrive(7, i, foreign)
        arrive(8, i, foreign)
        if foreign:
            moved_msg(2, i - POS).start()
            return
        pl.semaphore_wait(free_sem, 1)
        send(9, i, False)

    def stage6(i, foreign):
        if not foreign:
            arrive(9, i, False)

    plan = ((stage6, 16), (stage5, 14), (stage4, 11), (stage3, 8), (stage2, 5), (stage1, 2), (produce, 0))
    depth = max(lag for _, lag in plan)

    def run(i):
        for fn, lag in plan:
            j = i - lag
            live = (j >= 0) & (j < steps)

            @pl.when(live & jnp.logical_not(is_foreign(j)))
            def _():
                fn(j, False)

            if fn not in (produce, stage6):
                @pl.when(live & is_foreign(j))
                def _():
                    fn(j, True)

    def hand_over(i):
        @pl.when((i >= HAND) & (i < HAND + moved))
        def _():
            f = i - HAND
            c = total - moved + f
            acc_start(c, i % 2)
            acc_wait(i % 2)
            product(c, i % 2)
            moved_msg(0, f).start()

        @pl.when((i >= HAND + 2) & (i < HAND + 2 + moved))
        def _():
            f = i - HAND - 2
            c = total - moved + f
            moved_msg(0, f).wait_recv()
            p_s[c] = plus(p_s[c], m_ref[c, rows_of(hb, half), :])
            moved_msg(0, f).wait_send()
            pl.semaphore_signal(mv_free, inc=1, **dev(pp, pair))
            pl.semaphore_wait(z_free, 1)
            moved_msg(1, f).start()

    def give(i):
        f = i - (steps + depth - 2 - moved)

        @pl.when((f >= 0) & (f < moved))
        def _():
            moved_msg(2, f).wait_recv()
            pl.semaphore_wait(mv_free, 1)
            moved_msg(3, f).start()

    def step(i, carry):
        @pl.when(pp == 0)
        def _():
            @pl.when(i == EARLY)
            def _():
                layers(jnp.int32(stages - 1))
        run(i)

        @pl.when(jnp.logical_not(helper))
        def _():
            hand_over(i)
            give(i)
        return carry

    @pl.when(pp == 0)
    def _():
        cot_wait(stages - 1)
        keep_cot(stages - 1, 1, cot_now(stages - 1))
    lax.fori_loop(0, steps + depth, step, 0)

    @pl.when(jnp.logical_not(helper))
    def _():
        def take(f, carry):
            moved_msg(3, f, True).wait_recv()
            moved_msg(3, f).wait_send()
            moved_msg(1, f).wait_send()
            return carry
        lax.fori_loop(0, moved, take, 0)

    @pl.when(helper)
    def _():
        def back(f, carry):
            moved_msg(2, f).wait_send()
            return carry
        lax.fori_loop(0, moved, back, 0)

    def drain(i, carry):
        for kind in range(3, 10):
            msg(kind, steps - RING + i, False).wait_send()
        return carry

    lax.fori_loop(0, RING, drain, 0)

    @pl.when(pp > 0)
    def _():
        cot_wait(stages - 1)

    @pl.when(pp == stages - 1)
    def _():
        cot_wait(stages - 2)

    def sent(t, carry):
        for n in range(TILES):
            cot_copy(t, n).wait_send()
        return carry
    lax.fori_loop(0, stages - pp, sent, 0)
    out_slot = jnp.where(pp == 0, 0, stages - 1)
    for n in range(TILES):
        dx_ref[0, :, n * tile:(n + 1) * tile] = cb_s[out_slot, n]


def write_kernel(sizes, m_ref, dx_ref, gi_ref, go_ref, dxo_ref, out_s, out_sem, dx_sem):
    hid, ff, tok, stages = sizes
    cw = hid // COLS
    nq = ff // cw
    per_layer = 2 * nq
    total = 2 * per_layer
    slots = out_s.shape[0]
    dx_copy = pltpu.make_async_copy(dx_ref, dxo_ref, dx_sem)
    dx_copy.start()

    def copies(c):
        k = 1 - c // per_layer
        b = c % per_layer
        kind, jj = b // nq, b % nq
        slot = c % slots
        a = pltpu.make_async_copy(out_s.at[slot], go_ref.at[0, k, pl.ds(pl.multiple_of((jj // COLS) * hid, 128), hid), pl.ds(pl.multiple_of((jj % COLS) * cw, 128), cw)], out_sem.at[slot])
        b = pltpu.make_async_copy(out_s.at[slot], gi_ref.at[0, k, :, pl.ds(pl.multiple_of(jj * cw, 128), cw)], out_sem.at[slot])
        return kind, a, b

    def body(c, carry):
        @pl.when(c >= slots)
        def _():
            copies(c - slots)[2].wait()
        slot = c % slots
        nr = hid // 4
        for i in range(4):
            r = pl.ds(i * nr, nr)
            out_s[slot, r, :] = m_ref[c, r, :].astype(F32) * 0.125
        kind, a, b = copies(c)

        @pl.when(kind == 0)
        def _():
            a.start()

        @pl.when(kind == 1)
        def _():
            b.start()
        return carry

    lax.fori_loop(0, total, body, 0)

    def drain(i, carry):
        copies(total - slots + i)[2].wait()
        return carry
    lax.fori_loop(0, slots, drain, 0)
    dx_copy.wait()


def solution(mesh):
    stages = mesh.shape['pp']

    def device_fn(w_in, w_out, x_saved, h_saved, dy_in, acc_in, acc_out):
        hid, ff = w_in.shape[2:]
        tok = dy_in.shape[1]
        sizes = (hid, ff, tok, stages)
        cw = hid // COLS
        nq = ff // cw
        total = 4 * nq
        unit = hid // 16
        any_spec = pl.BlockSpec(memory_space=pltpu.HBM)
        vm_spec = pl.BlockSpec(memory_space=pltpu.VMEM)
        m_all, dx = pl.pallas_call(
            functools.partial(main_kernel, sizes),
            out_shape=(pltpu.VMEM((total, hid, cw), BF16), pltpu.VMEM((1, tok, hid), BF16)),
            in_specs=[any_spec] * 7,
            out_specs=(vm_spec, vm_spec),
            scratch_shapes=[
                pltpu.VMEM((2, ff // hid, hid, hid), BF16),
                pltpu.VMEM((2, ff, hid), BF16),
                pltpu.VMEM((2, 1 + ff // hid, hid, stages * tok), BF16),
                pltpu.VMEM((2, COLS + nq, stages, tok, cw), BF16),
                pltpu.VMEM((stages, 2, tok, hid), BF16),
                pltpu.VMEM((stages, TILES, tok, hid // TILES), BF16),
                pltpu.VMEM((2, hid, cw), F32),
                pltpu.VMEM((total, hid // 2, cw), BF16),
                pltpu.VMEM((total, 2, 2 * unit, cw), BF16),
                pltpu.VMEM((total, 2, unit, cw), BF16),
                pltpu.SemaphoreType.DMA((2, 2)),
                pltpu.SemaphoreType.DMA((stages // 2,)),
                pltpu.SemaphoreType.DMA,
                pltpu.SemaphoreType.DMA,
                pltpu.SemaphoreType.DMA((2,)),
                pltpu.SemaphoreType.DMA((stages, TILES)),
                pltpu.SemaphoreType.DMA((stages, TILES)),
                pltpu.SemaphoreType.DMA((10, RING)),
                pltpu.SemaphoreType.DMA((10, RECV_RING)),
                pltpu.SemaphoreType.REGULAR,
                pltpu.SemaphoreType.DMA((4, max(MOVED))),
                pltpu.SemaphoreType.DMA((4, max(MOVED))),
                pltpu.SemaphoreType.REGULAR,
                pltpu.SemaphoreType.REGULAR,
            ],
            compiler_params=pltpu.CompilerParams(collective_id=0, has_side_effects=True, vmem_limit_bytes=46900 * 1024),
            name='chain_reduce',
        )(w_in, w_out, x_saved, h_saved, dy_in, acc_in, acc_out)
        grad_in, grad_out, dx = pl.pallas_call(
            functools.partial(write_kernel, sizes),
            out_shape=(jax.ShapeDtypeStruct((1, 2, hid, ff), F32), jax.ShapeDtypeStruct((1, 2, ff, hid), F32), jax.ShapeDtypeStruct((1, tok, hid), BF16)),
            in_specs=[vm_spec, vm_spec],
            out_specs=(any_spec, any_spec, any_spec),
            scratch_shapes=[pltpu.VMEM((4, hid, cw), F32), pltpu.SemaphoreType.DMA((4,)), pltpu.SemaphoreType.DMA],
            compiler_params=pltpu.CompilerParams(vmem_limit_bytes=16 * 1024 * 1024),
            name='write_out',
        )(m_all, dx)
        return grad_in, grad_out, dx

    return jax.shard_map(device_fn, mesh=mesh, in_specs=(P('pp'), P('pp'), P('pp', None, None, 'dp'), P('pp', None, None, 'dp'), P('pp', 'dp'), P('pp', 'dp'), P('pp', 'dp')), out_specs=(P('pp'), P('pp'), P('pp', 'dp')), check_vma=False)
```

```python
import functools
import jax
import jax.numpy as jnp
from jax import lax
from jax.experimental import pallas as pl
from jax.experimental.pallas import tpu as pltpu
from jax.sharding import PartitionSpec as P

BF16 = jnp.bfloat16
F32 = jnp.float32
NT = (((1,), (1,)), ((), ()))
COLS = 3
TILES = 3
RING = 4
RECV_RING = 8
MOVED = (4, 2, 1, 5)
POS = 26
HAND = 13
EARLY = 10


def gelu_and_slope(h):
    root = 0.7978845608028654
    cube = 0.044715
    sq = h * h
    th = jnp.tanh(root * (h + cube * (h * sq)))
    cdf = 0.5 * (1.0 + th)
    slope = cdf + (0.5 * root) * h * (1.0 - th * th) * (1.0 + (3.0 * cube) * sq)
    return h * cdf, slope


def main_kernel(sizes, w_in, w_out, x_saved, h_saved, dy_in, acc_in, acc_out,
                m_ref, dx_ref,
                wi_s, wo_s, lt_s, rm_s, xs_s, cb_s, acc_s, p_s, h1_s, h2_s,
                wsem, hsem, xsem, dysem, accsem, cot_send, cot_recv,
                send_sem, recv_sem, free_sem, mv_send, mv_recv, z_free, mv_free):
    hid, ff, tok, stages = sizes
    cw = hid // COLS
    nq = ff // cw
    nb = ff // hid
    per_kind = nq
    per_layer = 2 * nq
    total = 2 * per_layer
    unit = hid // 16
    tile = hid // TILES
    rows4 = stages * tok

    pp = lax.axis_index('pp')
    dp = lax.axis_index('dp')
    core = dp % 2
    xc = (dp // 2) % 2
    yc = dp // 4
    pair = dp + 1 - 2 * core
    xn = dp + 2 - 4 * xc
    yn = dp + 4 - 8 * yc

    def dev(pp_i, dp_i):
        return dict(device_id=(pp_i, dp_i), device_id_type=pl.DeviceIdType.MESH)

    def w_out_copy(k):
        return pltpu.make_async_copy(w_out.at[0, k], wo_s.at[k], wsem.at[k, 0])

    def w_in_start(k):
        for j in range(nb):
            pltpu.make_async_copy(w_in.at[0, k, :, pl.ds(j * hid, hid)], wi_s.at[k, j], wsem.at[k, 1]).start()

    def w_in_wait(k):
        pltpu.make_async_copy(wi_s.at[k], wi_s.at[k], wsem.at[k, 1]).wait()

    def h_start(part):
        def one(i, carry):
            k = 1 - i // nq
            q = i % nq
            pltpu.make_async_copy(h_saved.at[0, pl.ds(2 * part, 2), k, :, pl.ds(pl.multiple_of(q * cw, 128), cw)],
                                  rm_s.at[k, COLS + q, pl.ds(2 * part, 2)], hsem.at[part]).start()
            return carry
        lax.fori_loop(0, 2 * nq, one, 0)

    def h_wait(part):
        where = rm_s.at[:, pl.ds(COLS, nq), pl.ds(2 * part, 2)]
        pltpu.make_async_copy(where, where, hsem.at[part]).wait()

    def dy_start():
        for n in range(TILES):
            pltpu.make_async_copy(dy_in.at[0, :, pl.ds(n * tile, tile)], cb_s.at[0, n], dysem).start()

    def dy_wait():
        pltpu.make_async_copy(cb_s.at[0], cb_s.at[0], dysem).wait()

    x_copy = pltpu.make_async_copy(x_saved.at[0], xs_s, xsem)

    def acc_where(c):
        k = 1 - c // per_layer
        b = c % per_layer
        return k, b // per_kind, b % per_kind

    def acc_copies(c, slot):
        k, kind, jj = acc_where(c)
        a = pltpu.make_async_copy(acc_out.at[0, 0, k, pl.ds(pl.multiple_of((jj // COLS) * hid, 128), hid), pl.ds(pl.multiple_of((jj % COLS) * cw, 128), cw)],
                                  acc_s.at[slot], accsem.at[slot])
        b = pltpu.make_async_copy(acc_in.at[0, 0, k, :, pl.ds(pl.multiple_of(jj * cw, 128), cw)], acc_s.at[slot], accsem.at[slot])
        return kind, a, b

    def acc_start(c, slot):
        kind, a, b = acc_copies(c, slot)

        @pl.when(kind == 0)
        def _():
            a.start()

        @pl.when(kind == 1)
        def _():
            b.start()

    def acc_wait(slot):
        pltpu.make_async_copy(acc_s.at[slot], acc_s.at[slot], accsem.at[slot]).wait()

    dy_start()
    h_start(0)
    w_out_copy(1).start()
    w_in_start(1)

    barrier = pltpu.get_barrier_semaphore()
    for other in (pair, xn, yn):
        pl.semaphore_signal(barrier, inc=1, **dev(pp, other))
    for step in range(1, stages):
        pl.semaphore_signal(barrier, inc=1, **dev((pp + step) % stages, dp))

    def cot_copy(t, n):
        above = pp > 0
        spare = (stages - 1, stages - 2) if isinstance(t, int) else (t, stages - 1)
        slot = jnp.where(above, t + 1, spare[1])
        return pltpu.make_async_remote_copy(src_ref=cb_s.at[t, n], dst_ref=cb_s.at[slot, n], send_sem=cot_send.at[t, n], recv_sem=cot_recv.at[slot, n],
                                            **dev(jnp.where(above, pp - 1, spare[0]), dp))

    def cot_arrival(t, n):
        return pltpu.make_async_remote_copy(src_ref=cb_s.at[t, n], dst_ref=cb_s.at[t, n], send_sem=cot_send.at[0, n], recv_sem=cot_recv.at[t, n],
                                            **dev(jnp.maximum(pp - 1, 0), dp))

    def cot_now(t):
        return jnp.concatenate([cb_s[t, n] for n in range(TILES)], axis=1)

    def keep_cot(t, k, cot):
        for j in range(COLS):
            rm_s[k, j, t] = cot[:, j * cw:(j + 1) * cw]

    def layer(t, k, sends):
        cot = cot_now(t)
        keep_cot(t, k, cot)
        for j in range(nb):
            e = lax.dot_general(cot, wo_s[k, j * hid:(j + 1) * hid, :], NT, preferred_element_type=F32)
            for i in range(COLS):
                q = j * COLS + i
                _, slope = gelu_and_slope(rm_s[k, COLS + q, t].astype(F32))
                rm_s[k, COLS + q, t] = (e[:, i * cw:(i + 1) * cw] * slope).astype(BF16)
        for n in range(TILES):
            back = cot[:, n * tile:(n + 1) * tile].astype(F32)
            for j in range(nb):
                dh = jnp.concatenate([rm_s[k, COLS + j * COLS + i, t] for i in range(COLS)], axis=1)
                back += lax.dot_general(dh, wi_s[k, j, n * tile:(n + 1) * tile, :], NT, preferred_element_type=F32)
            cb_s[t, n] = back.astype(BF16)
            if sends:
                cot_copy(t, n).start()

    def layers(t):
        layer(t, 1, False)
        layer(t, 0, True)

    def cot_wait(t):
        for n in range(TILES):
            cot_arrival(t, n).wait_recv()

    def prepare(k, carry):
        kept = [xs_s[t, k] * (pp + t < stages).astype(BF16) for t in range(stages)]
        lt_s[k, 0] = jnp.concatenate(kept, axis=0).T
        return carry

    def acts(part):
        def body(i, carry):
            k = 1 - i // nq
            q = i % nq
            hh = rm_s[k, COLS + q, 2 * part:2 * part + 2].reshape(2 * tok, cw).astype(F32)
            act, _ = gelu_and_slope(hh)
            act = jnp.where(lax.broadcasted_iota(jnp.int32, act.shape, 0) < (stages - pp - 2 * part) * tok, act, 0.0)
            lt_s[k, 1 + q // COLS, pl.ds(pl.multiple_of((q % COLS) * cw, 128), cw), 2 * part * tok:2 * (part + 1) * tok] = act.astype(BF16).T
            return carry
        lax.fori_loop(0, 2 * nq, body, 0)

    def zero_inactive(t, carry):
        zero = jnp.zeros((tok, cw), BF16)

        def one_layer(k, c2):
            for j in range(COLS):
                rm_s[k, j, t] = zero
            return c2
        return lax.fori_loop(0, 2, one_layer, carry)

    last = stages - 1 - pp
    uses_later = pp + 2 < stages

    @pl.when(jnp.logical_not(uses_later))
    def _():
        def blank(i, carry):
            k = i // nq
            q = i % nq
            rm_s[k, COLS + q, 2:] = jnp.zeros((stages - 2, tok, cw), BF16)
            lt_s[k, 1 + q // COLS, pl.ds(pl.multiple_of((q % COLS) * cw, 128), cw), 2 * tok:] = jnp.zeros((cw, (stages - 2) * tok), BF16)
            return carry
        lax.fori_loop(0, 2 * nq, blank, 0)
    lax.fori_loop(last + 1, stages, zero_inactive, 0)
    h_wait(0)
    w_out_copy(0).start()
    w_in_start(0)
    acts(0)
    dy_wait()
    pl.semaphore_wait(barrier, 3 + stages - 1)
    w_out_copy(1).wait()
    w_in_wait(1)
    layer(0, 1, False)
    x_copy.start()
    w_out_copy(0).wait()
    w_in_wait(0)
    layer(0, 0, True)
    acc_start(0, 0)

    @pl.when(uses_later)
    def _():
        h_start(1)
    x_copy.wait()
    lax.fori_loop(0, 2, prepare, 0)

    @pl.when(uses_later)
    def _():
        h_wait(1)

    def middle(t, carry):
        cot_wait(t)
        layers(t)

        @pl.when((t == 1) & uses_later)
        def _():
            acts(1)
        return carry

    lax.fori_loop(1, jnp.where(pp == 0, stages - 1, last + 1), middle, 0)

    half = hid // 2
    hb = core * half
    xb = hb
    yb = hb + 4 * unit
    helper = pp >= stages // 2
    moved = jnp.where(helper, jnp.where(pp == 2, MOVED[2], MOVED[3]), jnp.where(pp == 0, MOVED[0], MOVED[1]))
    steps = jnp.where(helper, total + moved, total - moved)
    own = jnp.where(helper, total, total - moved)

    def is_foreign(i):
        return helper & (i >= POS) & (i < POS + moved)

    def own_of(i):
        return jnp.where(helper & (i >= POS), i - moved, i)

    def rows_of(start, n):
        return pl.ds(pl.multiple_of(start, 16), n)

    def msg(kind, i, foreign, arriving=False):
        f = 1 if arriving else 0
        c = i - POS if foreign else own_of(i)

        def remote(src, dst, target):
            j = c if kind in (0, 9) else i
            row = (kind + 1) // 2
            return pltpu.make_async_remote_copy(src_ref=src, dst_ref=dst, send_sem=send_sem.at[row, j % RING], recv_sem=recv_sem.at[row, j % RECV_RING], **dev(pp, target))

        def place(start, n):
            return p_s.at[c, rows_of(start, n), :] if foreign else m_ref.at[c, rows_of(hb + start, n), :]
        yp = 4 * unit
        if kind == 0:
            return remote(m_ref.at[c, rows_of(half - hb, half), :], p_s.at[c], pair)
        if kind == 1:
            return remote(p_s.at[c, rows_of((1 - xc) * 2 * unit, 2 * unit), :], h1_s.at[c, 0], xn)
        if kind == 2:
            return remote(p_s.at[c, rows_of(yp + (1 - yc) * 2 * unit, 2 * unit), :], h1_s.at[c, 1], yn)
        if kind == 3:
            return remote(h1_s.at[c, 0, rows_of((1 - yc) * unit, unit), :], h2_s.at[c, 0], yn)
        if kind == 4:
            return remote(h1_s.at[c, 1, rows_of((1 - xc) * unit, unit), :], h2_s.at[c, 1], xn)
        if kind == 5:
            y_of = 1 - yc if f else yc
            r = place(xc * 2 * unit + y_of * unit, unit)
            return remote(r, r, yn)
        if kind == 6:
            x_of = 1 - xc if f else xc
            r = place(yp + yc * 2 * unit + x_of * unit, unit)
            return remote(r, r, xn)
        if kind == 7:
            x_of = 1 - xc if f else xc
            r = place(x_of * 2 * unit, 2 * unit)
            return remote(r, r, xn)
        if kind == 8:
            y_of = 1 - yc if f else yc
            r = place(yp + y_of * 2 * unit, 2 * unit)
            return remote(r, r, yn)
        r = m_ref.at[c, rows_of(half - hb if f else hb, half), :]
        return remote(r, r, pair)

    def taker(f):
        near = (pp == 1) & (f == 0)
        return jnp.where(near, 2, 3), jnp.where(pp == 0, f, jnp.where(near, 0, MOVED[0]))

    def giver(f):
        far = (pp == 3) & (f < MOVED[0])
        return jnp.where(far, 0, 1), jnp.where(far, f, jnp.where(pp == 3, 1, 0))

    def moved_msg(kind, f, arriving=False):
        c = total - moved + f

        def remote(src, dst, there, pp_i, dp_i):
            return pltpu.make_async_remote_copy(src_ref=src, dst_ref=dst, send_sem=mv_send.at[int(kind % 3 > 0), f], recv_sem=mv_recv.at[int(kind % 3 > 0), there], **dev(pp_i, dp_i))
        if kind == 0:
            return remote(m_ref.at[c, rows_of(half - hb, half), :], p_s.at[c], f, pp, pair)
        if kind == 1:
            if arriving:
                return remote(p_s.at[f], p_s.at[f], f, giver(f)[0], dp)
            stage, place = taker(f)
            return remote(p_s.at[c], p_s.at[place], place, stage, dp)
        if kind == 2:
            if arriving:
                return remote(p_s.at[f], m_ref.at[c, rows_of(hb, half), :], f, taker(f)[0], dp)
            stage, piece = giver(f)
            there = total - jnp.where(stage == 0, MOVED[0], MOVED[1]) + piece
            return remote(p_s.at[f], m_ref.at[there, rows_of(hb, half), :], piece, stage, dp)
        r = m_ref.at[c, rows_of(half - hb if arriving else hb, half), :]
        return remote(r, r, f, pp, pair)

    def bytes_of(kind):
        return {0: p_s, 1: h1_s, 3: h2_s, 5: h2_s, 7: h1_s, 9: p_s}[kind].at[0]

    def wait_on(sem, kind):
        place = bytes_of(kind)
        pltpu.make_async_copy(place, place, sem).wait()

    def wait_sent(kind, i):
        j = own_of(i) if kind in (0, 9) else i
        wait_on(send_sem.at[(kind + 1) // 2, j % RING], kind)

    def arrive(kind, i):
        j = own_of(i) if kind in (0, 9) else i
        wait_on(recv_sem.at[(kind + 1) // 2, j % RECV_RING], kind)

    def send(kind, i, foreign):
        if kind >= 3:
            j = own_of(i) if kind == 9 else i

            @pl.when(j >= RING)
            def _():
                wait_sent(kind, i)
        msg(kind, i, foreign).start()
        if kind not in (0, 9):
            msg(kind + 1, i, foreign).start()

    def plus(left, right):
        return (left.astype(F32) + right.astype(F32)).astype(BF16)

    def product(c, slot):
        k, kind, jj = acc_where(c)
        li = (1 - kind) * (1 + jj // COLS)
        ri = (1 - kind) * (jj % COLS) + kind * (COLS + jj)
        right = rm_s[k, ri].reshape(rows4, cw)
        nr = hid // 6 if hid % 768 == 0 else hid // 2
        for n in range(hid // nr):
            r = pl.ds(n * nr, nr)
            g = jnp.dot(lt_s[k, li, r, :], right, preferred_element_type=F32)
            m_ref[c, r, :] = (acc_s[slot, r, :] + g).astype(BF16)

    def produce(i, foreign):
        if foreign:
            return
        c = own_of(i)

        @pl.when(c + 1 < own)
        def _():
            acc_start(c + 1, (c + 1) % 2)
        acc_wait(c % 2)
        product(c, c % 2)
        send(0, i, False)

    def stage1(i, foreign):
        if foreign:
            f = i - POS
            moved_msg(1, f, True).wait_recv()
            send(1, i, True)
            return
        c = own_of(i)
        arrive(0, i)
        p_s[c] = plus(p_s[c], m_ref[c, rows_of(hb, half), :])
        send(1, i, False)
        wait_sent(0, i)
        pl.semaphore_signal(free_sem, inc=1, **dev(pp, pair))

    def stage2(i, foreign):
        c = i - POS if foreign else own_of(i)
        arrive(1, i)
        h1_s[c, 0] = plus(h1_s[c, 0], p_s[c, rows_of(xc * 2 * unit, 2 * unit), :])
        h1_s[c, 1] = plus(h1_s[c, 1], p_s[c, rows_of(4 * unit + yc * 2 * unit, 2 * unit), :])
        wait_sent(1, i)
        send(3, i, foreign)
        if not foreign:
            @pl.when(helper & (i < moved))
            def _():
                stage, piece = giver(i)
                pl.semaphore_signal(z_free.at[piece], inc=1, **dev(stage, dp))

    def stage3(i, foreign):
        c = i - POS if foreign else own_of(i)

        def keep(start, value):
            if foreign:
                p_s[c, rows_of(start, unit), :] = value
            else:
                m_ref[c, rows_of(hb + start, unit), :] = value
        arrive(3, i)
        keep(xc * 2 * unit + yc * unit, plus(h1_s[c, 0, rows_of(yc * unit, unit), :], h2_s[c, 0]))
        keep(4 * unit + yc * 2 * unit + xc * unit, plus(h1_s[c, 1, rows_of(xc * unit, unit), :], h2_s[c, 1]))
        send(5, i, foreign)

    def stage4(i, foreign):
        arrive(5, i)
        send(7, i, foreign)

    def stage5(i, foreign):
        arrive(7, i)
        if foreign:
            moved_msg(2, i - POS).start()
            return
        pl.semaphore_wait(free_sem, 1)
        send(9, i, False)

    def stage6(i, foreign):
        if not foreign:
            arrive(9, i)

    plan = ((stage6, 16), (stage5, 14), (stage4, 11), (stage3, 8), (stage2, 5), (stage1, 2), (produce, 0))
    depth = max(lag for _, lag in plan)

    def run(i):
        for fn, lag in plan:
            j = i - lag
            live = (j >= 0) & (j < steps)

            @pl.when(live & jnp.logical_not(is_foreign(j)))
            def _():
                fn(j, False)

            if fn not in (produce, stage6):
                @pl.when(live & is_foreign(j))
                def _():
                    fn(j, True)

    def hand_over(i):
        @pl.when((i >= HAND) & (i < HAND + moved))
        def _():
            f = i - HAND
            c = total - moved + f
            acc_start(c, i % 2)
            acc_wait(i % 2)
            product(c, i % 2)
            moved_msg(0, f).start()

        @pl.when((i >= HAND + 2) & (i < HAND + 2 + moved))
        def _():
            f = i - HAND - 2
            c = total - moved + f
            moved_msg(0, f).wait_recv()
            p_s[c] = plus(p_s[c], m_ref[c, rows_of(hb, half), :])
            moved_msg(0, f).wait_send()
            pl.semaphore_signal(mv_free, inc=1, **dev(pp, pair))
            pl.semaphore_wait(z_free.at[f], 1)
            moved_msg(1, f).start()

    def give(i):
        f = i - (steps + depth - 2 - moved)

        @pl.when((f >= 0) & (f < moved))
        def _():
            moved_msg(2, f, True).wait_recv()
            pl.semaphore_wait(mv_free, 1)
            moved_msg(3, f).start()

    def step(i, carry):
        @pl.when(pp == 0)
        def _():
            @pl.when(i == EARLY)
            def _():
                layers(jnp.int32(stages - 1))
        run(i)

        @pl.when(jnp.logical_not(helper))
        def _():
            hand_over(i)
            give(i)
        return carry

    @pl.when(pp == 0)
    def _():
        cot_wait(stages - 1)
        keep_cot(stages - 1, 1, cot_now(stages - 1))
    lax.fori_loop(0, steps + depth, step, 0)

    @pl.when(jnp.logical_not(helper))
    def _():
        def take(f, carry):
            moved_msg(3, f, True).wait_recv()
            moved_msg(3, f).wait_send()
            moved_msg(1, f).wait_send()
            return carry
        lax.fori_loop(0, moved, take, 0)

    @pl.when(helper)
    def _():
        def back(f, carry):
            moved_msg(2, f).wait_send()
            return carry
        lax.fori_loop(0, moved, back, 0)

    def drain(i, carry):
        for kind in (3, 5, 7, 9):
            wait_sent(kind, steps - RING + i)
        return carry

    lax.fori_loop(0, RING, drain, 0)

    @pl.when(pp > 0)
    def _():
        cot_wait(stages - 1)

    @pl.when(pp == stages - 1)
    def _():
        cot_wait(stages - 2)

    def sent(t, carry):
        for n in range(TILES):
            cot_copy(t, n).wait_send()
        return carry
    lax.fori_loop(0, stages - pp, sent, 0)
    out_slot = jnp.where(pp == 0, 0, stages - 1)
    for n in range(TILES):
        dx_ref[0, :, n * tile:(n + 1) * tile] = cb_s[out_slot, n]


def write_kernel(sizes, m_ref, dx_ref, gi_ref, go_ref, dxo_ref, out_s, out_sem, dx_sem):
    hid, ff, tok, stages = sizes
    cw = hid // COLS
    nq = ff // cw
    per_layer = 2 * nq
    total = 2 * per_layer
    slots = out_s.shape[0]
    dx_copy = pltpu.make_async_copy(dx_ref, dxo_ref, dx_sem)
    dx_copy.start()

    def copies(c):
        k = 1 - c // per_layer
        b = c % per_layer
        kind, jj = b // nq, b % nq
        slot = c % slots
        a = pltpu.make_async_copy(out_s.at[slot], go_ref.at[0, k, pl.ds(pl.multiple_of((jj // COLS) * hid, 128), hid), pl.ds(pl.multiple_of((jj % COLS) * cw, 128), cw)], out_sem.at[slot])
        b = pltpu.make_async_copy(out_s.at[slot], gi_ref.at[0, k, :, pl.ds(pl.multiple_of(jj * cw, 128), cw)], out_sem.at[slot])
        return kind, a, b

    def body(c, carry):
        @pl.when(c >= slots)
        def _():
            copies(c - slots)[2].wait()
        slot = c % slots
        nr = hid // 4
        for i in range(4):
            r = pl.ds(i * nr, nr)
            out_s[slot, r, :] = m_ref[c, r, :].astype(F32) * 0.125
        kind, a, b = copies(c)

        @pl.when(kind == 0)
        def _():
            a.start()

        @pl.when(kind == 1)
        def _():
            b.start()
        return carry

    lax.fori_loop(0, total, body, 0)

    def drain(i, carry):
        copies(total - slots + i)[2].wait()
        return carry
    lax.fori_loop(0, slots, drain, 0)
    dx_copy.wait()


def solution(mesh):
    stages = mesh.shape['pp']

    def device_fn(w_in, w_out, x_saved, h_saved, dy_in, acc_in, acc_out):
        hid, ff = w_in.shape[2:]
        tok = dy_in.shape[1]
        sizes = (hid, ff, tok, stages)
        cw = hid // COLS
        nq = ff // cw
        total = 4 * nq
        unit = hid // 16
        any_spec = pl.BlockSpec(memory_space=pltpu.HBM)
        vm_spec = pl.BlockSpec(memory_space=pltpu.VMEM)
        m_all, dx = pl.pallas_call(
            functools.partial(main_kernel, sizes),
            out_shape=(pltpu.VMEM((total, hid, cw), BF16), pltpu.VMEM((1, tok, hid), BF16)),
            in_specs=[any_spec] * 7,
            out_specs=(vm_spec, vm_spec),
            scratch_shapes=[
                pltpu.VMEM((2, ff // hid, hid, hid), BF16),
                pltpu.VMEM((2, ff, hid), BF16),
                pltpu.VMEM((2, 1 + ff // hid, hid, stages * tok), BF16),
                pltpu.VMEM((2, COLS + nq, stages, tok, cw), BF16),
                pltpu.VMEM((stages, 2, tok, hid), BF16),
                pltpu.VMEM((stages, TILES, tok, hid // TILES), BF16),
                pltpu.VMEM((2, hid, cw), F32),
                pltpu.VMEM((total, hid // 2, cw), BF16),
                pltpu.VMEM((total, 2, 2 * unit, cw), BF16),
                pltpu.VMEM((total, 2, unit, cw), BF16),
                pltpu.SemaphoreType.DMA((2, 2)),
                pltpu.SemaphoreType.DMA((stages // 2,)),
                pltpu.SemaphoreType.DMA,
                pltpu.SemaphoreType.DMA,
                pltpu.SemaphoreType.DMA((2,)),
                pltpu.SemaphoreType.DMA((stages, TILES)),
                pltpu.SemaphoreType.DMA((stages, TILES)),
                pltpu.SemaphoreType.DMA((6, RING)),
                pltpu.SemaphoreType.DMA((6, RECV_RING)),
                pltpu.SemaphoreType.REGULAR,
                pltpu.SemaphoreType.DMA((2, max(MOVED))),
                pltpu.SemaphoreType.DMA((2, max(MOVED))),
                pltpu.SemaphoreType.REGULAR((max(MOVED[:2]),)),
                pltpu.SemaphoreType.REGULAR,
            ],
            compiler_params=pltpu.CompilerParams(collective_id=0, has_side_effects=True, vmem_limit_bytes=46900 * 1024),
            name='chain_reduce',
        )(w_in, w_out, x_saved, h_saved, dy_in, acc_in, acc_out)
        grad_in, grad_out, dx = pl.pallas_call(
            functools.partial(write_kernel, sizes),
            out_shape=(jax.ShapeDtypeStruct((1, 2, hid, ff), F32), jax.ShapeDtypeStruct((1, 2, ff, hid), F32), jax.ShapeDtypeStruct((1, tok, hid), BF16)),
            in_specs=[vm_spec, vm_spec],
            out_specs=(any_spec, any_spec, any_spec),
            scratch_shapes=[pltpu.VMEM((4, hid, cw), F32), pltpu.SemaphoreType.DMA((4,)), pltpu.SemaphoreType.DMA],
            compiler_params=pltpu.CompilerParams(vmem_limit_bytes=16 * 1024 * 1024),
            name='write_out',
        )(m_all, dx)
        return grad_in, grad_out, dx

    return jax.shard_map(device_fn, mesh=mesh, in_specs=(P('pp'), P('pp'), P('pp', None, None, 'dp'), P('pp', None, None, 'dp'), P('pp', 'dp'), P('pp', 'dp'), P('pp', 'dp')), out_specs=(P('pp'), P('pp'), P('pp', 'dp')), check_vma=False)
```

```python
import functools
import jax
import jax.numpy as jnp
from jax import lax
from jax.experimental import pallas as pl
from jax.experimental.pallas import tpu as pltpu
from jax.sharding import PartitionSpec as P

BF16 = jnp.bfloat16
F32 = jnp.float32
NT = (((1,), (1,)), ((), ()))
COLS = 3
TILES = 3
RING = 4
RECV_RING = 8
MOVED = (3, 2, 1, 4)
POS = 26
HAND = 16
EARLY = (10, 15)
AHEAD = 2


def gelu_and_slope(h):
    root = 0.7978845608028654
    cube = 0.044715
    sq = h * h
    th = jnp.tanh(root * (h + cube * (h * sq)))
    cdf = 0.5 * (1.0 + th)
    slope = cdf + (0.5 * root) * h * (1.0 - th * th) * (1.0 + (3.0 * cube) * sq)
    return h * cdf, slope


def main_kernel(sizes, w_in, w_out, x_saved, h_saved, dy_in, acc_in, acc_out,
                m_ref, dx_ref,
                wi_s, wo_s, lt_s, rm_s, xs_s, cb_s, acc_s, p_s, h1_s, h2_s,
                wsem, hsem, xsem, dysem, accsem, cot_send, cot_recv,
                send_sem, recv_sem, free_sem, mv_send, mv_recv, z_free, mv_free):
    hid, ff, tok, stages = sizes
    cw = hid // COLS
    nq = ff // cw
    nb = ff // hid
    per_kind = nq
    per_layer = 2 * nq
    total = 2 * per_layer
    unit = hid // 16
    tile = hid // TILES
    rows4 = stages * tok

    pp = lax.axis_index('pp')
    dp = lax.axis_index('dp')
    core = dp % 2
    xc = (dp // 2) % 2
    yc = dp // 4
    pair = dp + 1 - 2 * core
    xn = dp + 2 - 4 * xc
    yn = dp + 4 - 8 * yc

    def dev(pp_i, dp_i):
        return dict(device_id=(pp_i, dp_i), device_id_type=pl.DeviceIdType.MESH)

    def w_out_copy(k):
        return pltpu.make_async_copy(w_out.at[0, k], wo_s.at[k], wsem.at[k, 0])

    def w_in_start(k):
        for j in range(nb):
            pltpu.make_async_copy(w_in.at[0, k, :, pl.ds(j * hid, hid)], wi_s.at[k, j], wsem.at[k, 1]).start()

    def w_in_wait(k):
        pltpu.make_async_copy(wi_s.at[k], wi_s.at[k], wsem.at[k, 1]).wait()

    def h_start(part):
        def one(i, carry):
            k = 1 - i // nq
            q = i % nq
            pltpu.make_async_copy(h_saved.at[0, pl.ds(2 * part, 2), k, :, pl.ds(pl.multiple_of(q * cw, 128), cw)],
                                  rm_s.at[k, COLS + q, pl.ds(2 * part, 2)], hsem.at[part]).start()
            return carry
        lax.fori_loop(0, 2 * nq, one, 0)

    def h_wait(part):
        where = rm_s.at[:, pl.ds(COLS, nq), pl.ds(2 * part, 2)]
        pltpu.make_async_copy(where, where, hsem.at[part]).wait()

    def dy_start():
        for n in range(TILES):
            pltpu.make_async_copy(dy_in.at[0, :, pl.ds(n * tile, tile)], cb_s.at[0, n], dysem).start()

    def dy_wait():
        pltpu.make_async_copy(cb_s.at[0], cb_s.at[0], dysem).wait()

    x_copy = pltpu.make_async_copy(x_saved.at[0], xs_s, xsem)

    def acc_where(c):
        k = 1 - c // per_layer
        b = c % per_layer
        return k, b // per_kind, b % per_kind

    def acc_copies(c, slot):
        k, kind, jj = acc_where(c)
        a = pltpu.make_async_copy(acc_out.at[0, 0, k, pl.ds(pl.multiple_of((jj // COLS) * hid, 128), hid), pl.ds(pl.multiple_of((jj % COLS) * cw, 128), cw)],
                                  acc_s.at[slot], accsem.at[slot])
        b = pltpu.make_async_copy(acc_in.at[0, 0, k, :, pl.ds(pl.multiple_of(jj * cw, 128), cw)], acc_s.at[slot], accsem.at[slot])
        return kind, a, b

    def acc_start(c, slot):
        kind, a, b = acc_copies(c, slot)

        @pl.when(kind == 0)
        def _():
            a.start()

        @pl.when(kind == 1)
        def _():
            b.start()

    def acc_wait(slot):
        pltpu.make_async_copy(acc_s.at[slot], acc_s.at[slot], accsem.at[slot]).wait()

    dy_start()
    h_start(0)
    w_out_copy(1).start()
    w_in_start(1)

    barrier = pltpu.get_barrier_semaphore()
    for other in (pair, xn, yn):
        pl.semaphore_signal(barrier, inc=1, **dev(pp, other))
    for step in range(1, stages):
        pl.semaphore_signal(barrier, inc=1, **dev((pp + step) % stages, dp))

    def cot_copy(t, n):
        above = pp > 0
        spare = (stages - 1, stages - 2) if isinstance(t, int) else (t, stages - 1)
        slot = jnp.where(above, t + 1, spare[1])
        return pltpu.make_async_remote_copy(src_ref=cb_s.at[t, n], dst_ref=cb_s.at[slot, n], send_sem=cot_send.at[t, n], recv_sem=cot_recv.at[slot, n],
                                            **dev(jnp.where(above, pp - 1, spare[0]), dp))

    def cot_arrival(t, n):
        return pltpu.make_async_remote_copy(src_ref=cb_s.at[t, n], dst_ref=cb_s.at[t, n], send_sem=cot_send.at[0, n], recv_sem=cot_recv.at[t, n],
                                            **dev(jnp.maximum(pp - 1, 0), dp))

    def cot_now(t):
        return jnp.concatenate([cb_s[t, n] for n in range(TILES)], axis=1)

    def keep_cot(t, k, cot):
        for j in range(COLS):
            rm_s[k, j, t] = cot[:, j * cw:(j + 1) * cw]

    def layer(t, k, sends):
        cot = cot_now(t)
        keep_cot(t, k, cot)
        for j in range(nb):
            e = lax.dot_general(cot, wo_s[k, j * hid:(j + 1) * hid, :], NT, preferred_element_type=F32)
            for i in range(COLS):
                q = j * COLS + i
                _, slope = gelu_and_slope(rm_s[k, COLS + q, t].astype(F32))
                rm_s[k, COLS + q, t] = (e[:, i * cw:(i + 1) * cw] * slope).astype(BF16)
        for n in range(TILES):
            back = cot[:, n * tile:(n + 1) * tile].astype(F32)
            for j in range(nb):
                dh = jnp.concatenate([rm_s[k, COLS + j * COLS + i, t] for i in range(COLS)], axis=1)
                back += lax.dot_general(dh, wi_s[k, j, n * tile:(n + 1) * tile, :], NT, preferred_element_type=F32)
            cb_s[t, n] = back.astype(BF16)
            if sends:
                cot_copy(t, n).start()

    def layers(t):
        layer(t, 1, False)
        layer(t, 0, True)

    def cot_wait(t):
        for n in range(TILES):
            cot_arrival(t, n).wait_recv()

    def prepare(k, carry):
        kept = [xs_s[t, k] * (pp + t < stages).astype(BF16) for t in range(stages)]
        lt_s[k, 0] = jnp.concatenate(kept, axis=0).T
        return carry

    def acts(part):
        def body(i, carry):
            k = 1 - i // nq
            q = i % nq
            hh = rm_s[k, COLS + q, 2 * part:2 * part + 2].reshape(2 * tok, cw).astype(F32)
            act, _ = gelu_and_slope(hh)
            act = jnp.where(lax.broadcasted_iota(jnp.int32, act.shape, 0) < (stages - pp - 2 * part) * tok, act, 0.0)
            lt_s[k, 1 + q // COLS, pl.ds(pl.multiple_of((q % COLS) * cw, 128), cw), 2 * part * tok:2 * (part + 1) * tok] = act.astype(BF16).T
            return carry
        lax.fori_loop(0, 2 * nq, body, 0)

    def zero_inactive(t, carry):
        zero = jnp.zeros((tok, cw), BF16)

        def one_layer(k, c2):
            for j in range(COLS):
                rm_s[k, j, t] = zero
            return c2
        return lax.fori_loop(0, 2, one_layer, carry)

    last = stages - 1 - pp
    uses_later = pp + 2 < stages

    @pl.when(jnp.logical_not(uses_later))
    def _():
        def blank(i, carry):
            k = i // nq
            q = i % nq
            rm_s[k, COLS + q, 2:] = jnp.zeros((stages - 2, tok, cw), BF16)
            lt_s[k, 1 + q // COLS, pl.ds(pl.multiple_of((q % COLS) * cw, 128), cw), 2 * tok:] = jnp.zeros((cw, (stages - 2) * tok), BF16)
            return carry
        lax.fori_loop(0, 2 * nq, blank, 0)
    lax.fori_loop(last + 1, stages, zero_inactive, 0)
    h_wait(0)
    w_out_copy(0).start()
    w_in_start(0)
    acts(0)
    dy_wait()
    pl.semaphore_wait(barrier, 3 + stages - 1)
    w_out_copy(1).wait()
    w_in_wait(1)
    layer(0, 1, False)
    x_copy.start()
    w_out_copy(0).wait()
    w_in_wait(0)
    for c in range(AHEAD):
        acc_start(c, c)
    layer(0, 0, True)

    @pl.when(uses_later)
    def _():
        h_start(1)
    x_copy.wait()
    lax.fori_loop(0, 2, prepare, 0)

    @pl.when(uses_later)
    def _():
        h_wait(1)

    def middle(t, carry):
        cot_wait(t)
        layers(t)

        @pl.when((t == 1) & uses_later)
        def _():
            acts(1)
        return carry

    lax.fori_loop(1, jnp.where(pp == 0, stages - 1, last + 1), middle, 0)

    half = hid // 2
    hb = core * half
    xb = hb
    yb = hb + 4 * unit
    helper = pp >= stages // 2
    moved = jnp.where(helper, jnp.where(pp == 2, MOVED[2], MOVED[3]), jnp.where(pp == 0, MOVED[0], MOVED[1]))
    steps = jnp.where(helper, total + moved, total - moved)
    own = jnp.where(helper, total, total - moved)

    def is_foreign(i):
        return helper & (i >= POS) & (i < POS + moved)

    def own_of(i):
        return jnp.where(helper & (i >= POS), i - moved, i)

    def rows_of(start, n):
        return pl.ds(pl.multiple_of(start, 16), n)

    def msg(kind, i, foreign, arriving=False):
        f = 1 if arriving else 0
        c = i - POS if foreign else own_of(i)

        def remote(src, dst, target):
            j = c if kind in (0, 9) else i
            row = (kind + 1) // 2
            return pltpu.make_async_remote_copy(src_ref=src, dst_ref=dst, send_sem=send_sem.at[row, j % RING], recv_sem=recv_sem.at[row, j % RECV_RING], **dev(pp, target))

        def place(start, n):
            return p_s.at[c, rows_of(start, n), :] if foreign else m_ref.at[c, rows_of(hb + start, n), :]
        yp = 4 * unit
        if kind == 0:
            return remote(m_ref.at[c, rows_of(half - hb, half), :], p_s.at[c], pair)
        if kind == 1:
            return remote(p_s.at[c, rows_of((1 - xc) * 2 * unit, 2 * unit), :], h1_s.at[c, 0], xn)
        if kind == 2:
            return remote(p_s.at[c, rows_of(yp + (1 - yc) * 2 * unit, 2 * unit), :], h1_s.at[c, 1], yn)
        if kind == 3:
            return remote(h1_s.at[c, 0, rows_of((1 - yc) * unit, unit), :], h2_s.at[c, 0], yn)
        if kind == 4:
            return remote(h1_s.at[c, 1, rows_of((1 - xc) * unit, unit), :], h2_s.at[c, 1], xn)
        if kind == 5:
            y_of = 1 - yc if f else yc
            r = place(xc * 2 * unit + y_of * unit, unit)
            return remote(r, r, yn)
        if kind == 6:
            x_of = 1 - xc if f else xc
            r = place(yp + yc * 2 * unit + x_of * unit, unit)
            return remote(r, r, xn)
        if kind == 7:
            x_of = 1 - xc if f else xc
            r = place(x_of * 2 * unit, 2 * unit)
            return remote(r, r, xn)
        if kind == 8:
            y_of = 1 - yc if f else yc
            r = place(yp + y_of * 2 * unit, 2 * unit)
            return remote(r, r, yn)
        r = m_ref.at[c, rows_of(half - hb if f else hb, half), :]
        return remote(r, r, pair)

    def taker(f):
        near = (pp == 1) & (f == 0)
        return jnp.where(near, 2, 3), jnp.where(pp == 0, f, jnp.where(near, 0, MOVED[0]))

    def giver(f):
        far = (pp == 3) & (f < MOVED[0])
        return jnp.where(far, 0, 1), jnp.where(far, f, jnp.where(pp == 3, 1, 0))

    def moved_msg(kind, f, arriving=False):
        c = total - moved + f

        def remote(src, dst, there, pp_i, dp_i):
            return pltpu.make_async_remote_copy(src_ref=src, dst_ref=dst, send_sem=mv_send.at[int(kind % 3 > 0), f], recv_sem=mv_recv.at[int(kind % 3 > 0), there], **dev(pp_i, dp_i))
        if kind == 0:
            return remote(m_ref.at[c, rows_of(half - hb, half), :], p_s.at[c], f, pp, pair)
        if kind == 1:
            if arriving:
                return remote(p_s.at[f], p_s.at[f], f, giver(f)[0], dp)
            stage, place = taker(f)
            return remote(p_s.at[c], p_s.at[place], place, stage, dp)
        if kind == 2:
            if arriving:
                return remote(p_s.at[f], m_ref.at[c, rows_of(hb, half), :], f, taker(f)[0], dp)
            stage, piece = giver(f)
            there = total - jnp.where(stage == 0, MOVED[0], MOVED[1]) + piece
            return remote(p_s.at[f], m_ref.at[there, rows_of(hb, half), :], piece, stage, dp)
        r = m_ref.at[c, rows_of(half - hb if arriving else hb, half), :]
        return remote(r, r, f, pp, pair)

    def bytes_of(kind):
        return {0: p_s, 1: h1_s, 3: h2_s, 5: h2_s, 7: h1_s, 9: p_s}[kind].at[0]

    def wait_on(sem, kind):
        place = bytes_of(kind)
        pltpu.make_async_copy(place, place, sem).wait()

    def wait_sent(kind, i):
        j = own_of(i) if kind in (0, 9) else i
        wait_on(send_sem.at[(kind + 1) // 2, j % RING], kind)

    def arrive(kind, i):
        j = own_of(i) if kind in (0, 9) else i
        wait_on(recv_sem.at[(kind + 1) // 2, j % RECV_RING], kind)

    def send(kind, i, foreign):
        if kind >= 3:
            j = own_of(i) if kind == 9 else i

            @pl.when(j >= RING)
            def _():
                wait_sent(kind, i)
        msg(kind, i, foreign).start()
        if kind not in (0, 9):
            msg(kind + 1, i, foreign).start()

    def plus(left, right):
        return (left.astype(F32) + right.astype(F32)).astype(BF16)

    def product(c, slot):
        k, kind, jj = acc_where(c)
        li = (1 - kind) * (1 + jj // COLS)
        ri = (1 - kind) * (jj % COLS) + kind * (COLS + jj)
        right = rm_s[k, ri].reshape(rows4, cw)
        nr = hid // 6 if hid % 768 == 0 else hid // 2
        for n in range(hid // nr):
            r = pl.ds(n * nr, nr)
            g = jnp.dot(lt_s[k, li, r, :], right, preferred_element_type=F32)
            m_ref[c, r, :] = (acc_s[slot, r, :] + g).astype(BF16)

    def produce(i, foreign):
        if foreign:
            return
        c = own_of(i)

        @pl.when(c + AHEAD < own)
        def _():
            acc_start(c + AHEAD, (c + AHEAD) % (AHEAD + 1))
        acc_wait(c % (AHEAD + 1))
        product(c, c % (AHEAD + 1))
        send(0, i, False)

    def stage1(i, foreign):
        if foreign:
            f = i - POS
            moved_msg(1, f, True).wait_recv()
            send(1, i, True)
            return
        c = own_of(i)
        arrive(0, i)
        p_s[c] = plus(p_s[c], m_ref[c, rows_of(hb, half), :])
        send(1, i, False)
        wait_sent(0, i)
        pl.semaphore_signal(free_sem, inc=1, **dev(pp, pair))

    def stage2(i, foreign):
        c = i - POS if foreign else own_of(i)
        arrive(1, i)
        h1_s[c, 0] = plus(h1_s[c, 0], p_s[c, rows_of(xc * 2 * unit, 2 * unit), :])
        h1_s[c, 1] = plus(h1_s[c, 1], p_s[c, rows_of(4 * unit + yc * 2 * unit, 2 * unit), :])
        wait_sent(1, i)
        send(3, i, foreign)
        if not foreign:
            @pl.when(helper & (i < moved))
            def _():
                stage, piece = giver(i)
                pl.semaphore_signal(z_free.at[piece], inc=1, **dev(stage, dp))

    def stage3(i, foreign):
        c = i - POS if foreign else own_of(i)

        def keep(start, value):
            if foreign:
                p_s[c, rows_of(start, unit), :] = value
            else:
                m_ref[c, rows_of(hb + start, unit), :] = value
        arrive(3, i)
        keep(xc * 2 * unit + yc * unit, plus(h1_s[c, 0, rows_of(yc * unit, unit), :], h2_s[c, 0]))
        keep(4 * unit + yc * 2 * unit + xc * unit, plus(h1_s[c, 1, rows_of(xc * unit, unit), :], h2_s[c, 1]))
        send(5, i, foreign)

    def stage4(i, foreign):
        arrive(5, i)
        send(7, i, foreign)

    def stage5(i, foreign):
        arrive(7, i)
        if foreign:
            moved_msg(2, i - POS).start()
            return
        pl.semaphore_wait(free_sem, 1)
        send(9, i, False)

    def stage6(i, foreign):
        if not foreign:
            arrive(9, i)

    plan = ((stage6, 16), (stage5, 14), (stage4, 11), (stage3, 8), (stage2, 5), (stage1, 2), (produce, 0))
    depth = max(lag for _, lag in plan)

    def run(i):
        for fn, lag in plan:
            j = i - lag
            live = (j >= 0) & (j < steps)

            @pl.when(live & jnp.logical_not(is_foreign(j)))
            def _():
                fn(j, False)

            if fn not in (produce, stage6):
                @pl.when(live & is_foreign(j))
                def _():
                    fn(j, True)

    def hand_over(i):
        @pl.when((i >= HAND) & (i < HAND + moved))
        def _():
            f = i - HAND
            c = total - moved + f
            acc_start(c, i % (AHEAD + 1))
            acc_wait(i % (AHEAD + 1))
            product(c, i % (AHEAD + 1))
            moved_msg(0, f).start()

        @pl.when((i >= HAND + 2) & (i < HAND + 2 + moved))
        def _():
            f = i - HAND - 2
            c = total - moved + f
            moved_msg(0, f).wait_recv()
            p_s[c] = plus(p_s[c], m_ref[c, rows_of(hb, half), :])
            moved_msg(0, f).wait_send()
            pl.semaphore_signal(mv_free, inc=1, **dev(pp, pair))
            pl.semaphore_wait(z_free.at[f], 1)
            moved_msg(1, f).start()

    def give(i):
        f = i - (steps + depth - 2 - moved)

        @pl.when((f >= 0) & (f < moved))
        def _():
            moved_msg(2, f, True).wait_recv()
            pl.semaphore_wait(mv_free, 1)
            moved_msg(3, f).start()

    def step(i, carry):
        @pl.when(pp == 0)
        def _():
            @pl.when(i == EARLY[0])
            def _():
                layer(jnp.int32(stages - 1), 1, False)

            @pl.when(i == EARLY[1])
            def _():
                layer(jnp.int32(stages - 1), 0, True)
        run(i)

        @pl.when(jnp.logical_not(helper))
        def _():
            hand_over(i)
            give(i)
        return carry

    @pl.when(pp == 0)
    def _():
        cot_wait(stages - 1)
        keep_cot(stages - 1, 1, cot_now(stages - 1))
    lax.fori_loop(0, steps + depth, step, 0)

    @pl.when(jnp.logical_not(helper))
    def _():
        def take(f, carry):
            moved_msg(3, f, True).wait_recv()
            moved_msg(3, f).wait_send()
            moved_msg(1, f).wait_send()
            return carry
        lax.fori_loop(0, moved, take, 0)

    @pl.when(helper)
    def _():
        def back(f, carry):
            moved_msg(2, f).wait_send()
            return carry
        lax.fori_loop(0, moved, back, 0)

    def drain(i, carry):
        for kind in (3, 5, 7, 9):
            wait_sent(kind, steps - RING + i)
        return carry

    lax.fori_loop(0, RING, drain, 0)

    @pl.when(pp > 0)
    def _():
        cot_wait(stages - 1)

    @pl.when(pp == stages - 1)
    def _():
        cot_wait(stages - 2)

    def sent(t, carry):
        for n in range(TILES):
            cot_copy(t, n).wait_send()
        return carry
    lax.fori_loop(0, stages - pp, sent, 0)
    out_slot = jnp.where(pp == 0, 0, stages - 1)
    for n in range(TILES):
        dx_ref[0, :, n * tile:(n + 1) * tile] = cb_s[out_slot, n]


def write_kernel(sizes, m_ref, dx_ref, gi_ref, go_ref, dxo_ref, out_s, out_sem, dx_sem):
    hid, ff, tok, stages = sizes
    cw = hid // COLS
    nq = ff // cw
    per_layer = 2 * nq
    total = 2 * per_layer
    slots = out_s.shape[0]
    dx_copy = pltpu.make_async_copy(dx_ref, dxo_ref, dx_sem)
    dx_copy.start()

    def copies(c):
        k = 1 - c // per_layer
        b = c % per_layer
        kind, jj = b // nq, b % nq
        slot = c % slots
        a = pltpu.make_async_copy(out_s.at[slot], go_ref.at[0, k, pl.ds(pl.multiple_of((jj // COLS) * hid, 128), hid), pl.ds(pl.multiple_of((jj % COLS) * cw, 128), cw)], out_sem.at[slot])
        b = pltpu.make_async_copy(out_s.at[slot], gi_ref.at[0, k, :, pl.ds(pl.multiple_of(jj * cw, 128), cw)], out_sem.at[slot])
        return kind, a, b

    def body(c, carry):
        @pl.when(c >= slots)
        def _():
            copies(c - slots)[2].wait()
        slot = c % slots
        nr = hid // 4
        for i in range(4):
            r = pl.ds(i * nr, nr)
            out_s[slot, r, :] = m_ref[c, r, :].astype(F32) * 0.125
        kind, a, b = copies(c)

        @pl.when(kind == 0)
        def _():
            a.start()

        @pl.when(kind == 1)
        def _():
            b.start()
        return carry

    lax.fori_loop(0, total, body, 0)

    def drain(i, carry):
        copies(total - slots + i)[2].wait()
        return carry
    lax.fori_loop(0, slots, drain, 0)
    dx_copy.wait()


def solution(mesh):
    stages = mesh.shape['pp']

    def device_fn(w_in, w_out, x_saved, h_saved, dy_in, acc_in, acc_out):
        hid, ff = w_in.shape[2:]
        tok = dy_in.shape[1]
        sizes = (hid, ff, tok, stages)
        cw = hid // COLS
        nq = ff // cw
        total = 4 * nq
        unit = hid // 16
        any_spec = pl.BlockSpec(memory_space=pltpu.HBM)
        vm_spec = pl.BlockSpec(memory_space=pltpu.VMEM)
        m_all, dx = pl.pallas_call(
            functools.partial(main_kernel, sizes),
            out_shape=(pltpu.VMEM((total, hid, cw), BF16), pltpu.VMEM((1, tok, hid), BF16)),
            in_specs=[any_spec] * 7,
            out_specs=(vm_spec, vm_spec),
            scratch_shapes=[
                pltpu.VMEM((2, ff // hid, hid, hid), BF16),
                pltpu.VMEM((2, ff, hid), BF16),
                pltpu.VMEM((2, 1 + ff // hid, hid, stages * tok), BF16),
                pltpu.VMEM((2, COLS + nq, stages, tok, cw), BF16),
                pltpu.VMEM((stages, 2, tok, hid), BF16),
                pltpu.VMEM((stages, TILES, tok, hid // TILES), BF16),
                pltpu.VMEM((AHEAD + 1, hid, cw), F32),
                pltpu.VMEM((total, hid // 2, cw), BF16),
                pltpu.VMEM((total, 2, 2 * unit, cw), BF16),
                pltpu.VMEM((total, 2, unit, cw), BF16),
                pltpu.SemaphoreType.DMA((2, 2)),
                pltpu.SemaphoreType.DMA((stages // 2,)),
                pltpu.SemaphoreType.DMA,
                pltpu.SemaphoreType.DMA,
                pltpu.SemaphoreType.DMA((AHEAD + 1,)),
                pltpu.SemaphoreType.DMA((stages, TILES)),
                pltpu.SemaphoreType.DMA((stages, TILES)),
                pltpu.SemaphoreType.DMA((6, RING)),
                pltpu.SemaphoreType.DMA((6, RECV_RING)),
                pltpu.SemaphoreType.REGULAR,
                pltpu.SemaphoreType.DMA((2, max(MOVED))),
                pltpu.SemaphoreType.DMA((2, max(MOVED))),
                pltpu.SemaphoreType.REGULAR((max(MOVED[:2]),)),
                pltpu.SemaphoreType.REGULAR,
            ],
            compiler_params=pltpu.CompilerParams(collective_id=0, has_side_effects=True, vmem_limit_bytes=46900 * 1024),
            name='chain_reduce',
        )(w_in, w_out, x_saved, h_saved, dy_in, acc_in, acc_out)
        grad_in, grad_out, dx = pl.pallas_call(
            functools.partial(write_kernel, sizes),
            out_shape=(jax.ShapeDtypeStruct((1, 2, hid, ff), F32), jax.ShapeDtypeStruct((1, 2, ff, hid), F32), jax.ShapeDtypeStruct((1, tok, hid), BF16)),
            in_specs=[vm_spec, vm_spec],
            out_specs=(any_spec, any_spec, any_spec),
            scratch_shapes=[pltpu.VMEM((4, hid, cw), F32), pltpu.SemaphoreType.DMA((4,)), pltpu.SemaphoreType.DMA],
            compiler_params=pltpu.CompilerParams(vmem_limit_bytes=16 * 1024 * 1024),
            name='write_out',
        )(m_all, dx)
        return grad_in, grad_out, dx

    return jax.shard_map(device_fn, mesh=mesh, in_specs=(P('pp'), P('pp'), P('pp', None, None, 'dp'), P('pp', None, None, 'dp'), P('pp', 'dp'), P('pp', 'dp'), P('pp', 'dp')), out_specs=(P('pp'), P('pp'), P('pp', 'dp')), check_vma=False)
```

```python
import functools
import jax
import jax.numpy as jnp
from jax import lax
from jax.experimental import pallas as pl
from jax.experimental.pallas import tpu as pltpu
from jax.sharding import PartitionSpec as P

BF16 = jnp.bfloat16
F32 = jnp.float32
NT = (((1,), (1,)), ((), ()))
COLS = 3
TILES = 3
RING = 4
RECV_RING = 8
MOVED = (3, 2, 1, 4)
POS = 34
HAND = 20
EARLY = (10, 15)
AHEAD = 2


def gelu_and_slope(h):
    root = 0.7978845608028654
    cube = 0.044715
    sq = h * h
    th = jnp.tanh(root * (h + cube * (h * sq)))
    cdf = 0.5 * (1.0 + th)
    slope = cdf + (0.5 * root) * h * (1.0 - th * th) * (1.0 + (3.0 * cube) * sq)
    return h * cdf, slope


def main_kernel(sizes, w_in, w_out, x_saved, h_saved, dy_in, acc_in, acc_out,
                m_ref, dx_ref,
                wi_s, wo_s, lt_s, rm_s, xs_s, cb_s, acc_s, p_s, h1_s, h2_s,
                wsem, hsem, xsem, dysem, accsem, cot_send, cot_recv,
                send_sem, recv_sem, free_sem, mv_send, mv_recv, z_free, mv_free):
    hid, ff, tok, stages = sizes
    cw = hid // COLS
    nq = ff // cw
    nb = ff // hid
    per_kind = nq
    per_layer = 2 * nq
    total = 2 * per_layer
    unit = hid // 16
    tile = hid // TILES
    rows4 = stages * tok

    pp = lax.axis_index('pp')
    dp = lax.axis_index('dp')
    core = dp % 2
    xc = (dp // 2) % 2
    yc = dp // 4
    pair = dp + 1 - 2 * core
    xn = dp + 2 - 4 * xc
    yn = dp + 4 - 8 * yc

    def dev(pp_i, dp_i):
        return dict(device_id=(pp_i, dp_i), device_id_type=pl.DeviceIdType.MESH)

    def w_out_copy(k):
        return pltpu.make_async_copy(w_out.at[0, k], wo_s.at[k], wsem.at[k, 0])

    def w_in_start(k):
        for j in range(nb):
            pltpu.make_async_copy(w_in.at[0, k, :, pl.ds(j * hid, hid)], wi_s.at[k, j], wsem.at[k, 1]).start()

    def w_in_wait(k):
        pltpu.make_async_copy(wi_s.at[k], wi_s.at[k], wsem.at[k, 1]).wait()

    def h_start(part):
        def one(i, carry):
            k = 1 - i // nq
            q = i % nq
            pltpu.make_async_copy(h_saved.at[0, pl.ds(2 * part, 2), k, :, pl.ds(pl.multiple_of(q * cw, 128), cw)],
                                  rm_s.at[k, COLS + q, pl.ds(2 * part, 2)], hsem.at[part]).start()
            return carry
        lax.fori_loop(0, 2 * nq, one, 0)

    def h_wait(part):
        where = rm_s.at[:, pl.ds(COLS, nq), pl.ds(2 * part, 2)]
        pltpu.make_async_copy(where, where, hsem.at[part]).wait()

    def dy_start():
        for n in range(TILES):
            pltpu.make_async_copy(dy_in.at[0, :, pl.ds(n * tile, tile)], cb_s.at[0, n], dysem).start()

    def dy_wait():
        pltpu.make_async_copy(cb_s.at[0], cb_s.at[0], dysem).wait()

    x_copy = pltpu.make_async_copy(x_saved.at[0], xs_s, xsem)

    def acc_where(c):
        k = 1 - c // per_layer
        b = c % per_layer
        return k, b // per_kind, b % per_kind

    def acc_copies(c, slot):
        k, kind, jj = acc_where(c)
        a = pltpu.make_async_copy(acc_out.at[0, 0, k, pl.ds(pl.multiple_of((jj // COLS) * hid, 128), hid), pl.ds(pl.multiple_of((jj % COLS) * cw, 128), cw)],
                                  acc_s.at[slot], accsem.at[slot])
        b = pltpu.make_async_copy(acc_in.at[0, 0, k, :, pl.ds(pl.multiple_of(jj * cw, 128), cw)], acc_s.at[slot], accsem.at[slot])
        return kind, a, b

    def acc_start(c, slot):
        kind, a, b = acc_copies(c, slot)

        @pl.when(kind == 0)
        def _():
            a.start()

        @pl.when(kind == 1)
        def _():
            b.start()

    def acc_wait(slot):
        pltpu.make_async_copy(acc_s.at[slot], acc_s.at[slot], accsem.at[slot]).wait()

    dy_start()
    h_start(0)
    w_out_copy(1).start()
    w_in_start(1)

    barrier = pltpu.get_barrier_semaphore()
    for other in (pair, xn, yn):
        pl.semaphore_signal(barrier, inc=1, **dev(pp, other))
    for step in range(1, stages):
        pl.semaphore_signal(barrier, inc=1, **dev((pp + step) % stages, dp))

    def cot_copy(t, n):
        above = pp > 0
        spare = (stages - 1, stages - 2) if isinstance(t, int) else (t, stages - 1)
        slot = jnp.where(above, t + 1, spare[1])
        return pltpu.make_async_remote_copy(src_ref=cb_s.at[t, n], dst_ref=cb_s.at[slot, n], send_sem=cot_send.at[t, n], recv_sem=cot_recv.at[slot, n],
                                            **dev(jnp.where(above, pp - 1, spare[0]), dp))

    def cot_arrival(t, n):
        return pltpu.make_async_remote_copy(src_ref=cb_s.at[t, n], dst_ref=cb_s.at[t, n], send_sem=cot_send.at[0, n], recv_sem=cot_recv.at[t, n],
                                            **dev(jnp.maximum(pp - 1, 0), dp))

    def cot_now(t):
        return jnp.concatenate([cb_s[t, n] for n in range(TILES)], axis=1)

    def keep_cot(t, k, cot):
        for j in range(COLS):
            rm_s[k, j, t] = cot[:, j * cw:(j + 1) * cw]

    def layer(t, k, sends):
        cot = cot_now(t)
        keep_cot(t, k, cot)
        for j in range(nb):
            e = lax.dot_general(cot, wo_s[k, j * hid:(j + 1) * hid, :], NT, preferred_element_type=F32)
            for i in range(COLS):
                q = j * COLS + i
                _, slope = gelu_and_slope(rm_s[k, COLS + q, t].astype(F32))
                rm_s[k, COLS + q, t] = (e[:, i * cw:(i + 1) * cw] * slope).astype(BF16)
        for n in range(TILES):
            back = cot[:, n * tile:(n + 1) * tile].astype(F32)
            for j in range(nb):
                dh = jnp.concatenate([rm_s[k, COLS + j * COLS + i, t] for i in range(COLS)], axis=1)
                back += lax.dot_general(dh, wi_s[k, j, n * tile:(n + 1) * tile, :], NT, preferred_element_type=F32)
            cb_s[t, n] = back.astype(BF16)
            if sends:
                cot_copy(t, n).start()

    def layers(t):
        layer(t, 1, False)
        layer(t, 0, True)

    def cot_wait(t):
        for n in range(TILES):
            cot_arrival(t, n).wait_recv()

    def prepare(k, carry):
        kept = [xs_s[t, k] * (pp + t < stages).astype(BF16) for t in range(stages)]
        lt_s[k, 0] = jnp.concatenate(kept, axis=0).T
        return carry

    def acts(part):
        def body(i, carry):
            k = 1 - i // nq
            q = i % nq
            hh = rm_s[k, COLS + q, 2 * part:2 * part + 2].reshape(2 * tok, cw).astype(F32)
            act, _ = gelu_and_slope(hh)
            act = jnp.where(lax.broadcasted_iota(jnp.int32, act.shape, 0) < (stages - pp - 2 * part) * tok, act, 0.0)
            lt_s[k, 1 + q // COLS, pl.ds(pl.multiple_of((q % COLS) * cw, 128), cw), 2 * part * tok:2 * (part + 1) * tok] = act.astype(BF16).T
            return carry
        lax.fori_loop(0, 2 * nq, body, 0)

    def zero_inactive(t, carry):
        zero = jnp.zeros((tok, cw), BF16)

        def one_layer(k, c2):
            for j in range(COLS):
                rm_s[k, j, t] = zero
            return c2
        return lax.fori_loop(0, 2, one_layer, carry)

    last = stages - 1 - pp
    uses_later = pp + 2 < stages

    @pl.when(jnp.logical_not(uses_later))
    def _():
        def blank(i, carry):
            k = i // nq
            q = i % nq
            rm_s[k, COLS + q, 2:] = jnp.zeros((stages - 2, tok, cw), BF16)
            lt_s[k, 1 + q // COLS, pl.ds(pl.multiple_of((q % COLS) * cw, 128), cw), 2 * tok:] = jnp.zeros((cw, (stages - 2) * tok), BF16)
            return carry
        lax.fori_loop(0, 2 * nq, blank, 0)
    lax.fori_loop(last + 1, stages, zero_inactive, 0)
    h_wait(0)
    w_out_copy(0).start()
    w_in_start(0)
    acts(0)
    dy_wait()
    pl.semaphore_wait(barrier, 3 + stages - 1)
    w_out_copy(1).wait()
    w_in_wait(1)
    layer(0, 1, False)
    x_copy.start()
    w_out_copy(0).wait()
    w_in_wait(0)
    for c in range(AHEAD):
        acc_start(c, c)
    layer(0, 0, True)

    @pl.when(uses_later)
    def _():
        h_start(1)
    x_copy.wait()
    lax.fori_loop(0, 2, prepare, 0)

    @pl.when(uses_later)
    def _():
        h_wait(1)

    def middle(t, carry):
        cot_wait(t)
        layers(t)

        @pl.when((t == 1) & uses_later)
        def _():
            acts(1)
        return carry

    lax.fori_loop(1, jnp.where(pp == 0, stages - 1, last + 1), middle, 0)

    half = hid // 2
    hb = core * half
    xb = hb
    yb = hb + 4 * unit
    helper = pp >= stages // 2
    moved = jnp.where(helper, jnp.where(pp == 2, MOVED[2], MOVED[3]), jnp.where(pp == 0, MOVED[0], MOVED[1]))
    steps = jnp.where(helper, total + moved, total - moved)
    own = jnp.where(helper, total, total - moved)

    def is_foreign(i):
        return helper & (i >= POS) & (i < POS + moved)

    def own_of(i):
        return jnp.where(helper & (i >= POS), i - moved, i)

    def rows_of(start, n):
        return pl.ds(pl.multiple_of(start, 16), n)

    def msg(kind, i, foreign, arriving=False):
        f = 1 if arriving else 0
        c = i - POS if foreign else own_of(i)

        def remote(src, dst, target):
            j = c if kind in (0, 9) else i
            row = (kind + 1) // 2
            return pltpu.make_async_remote_copy(src_ref=src, dst_ref=dst, send_sem=send_sem.at[row, j % RING], recv_sem=recv_sem.at[row, j % RECV_RING], **dev(pp, target))

        def place(start, n):
            return p_s.at[c, rows_of(start, n), :] if foreign else m_ref.at[c, rows_of(hb + start, n), :]
        yp = 4 * unit
        if kind == 0:
            return remote(m_ref.at[c, rows_of(half - hb, half), :], p_s.at[c], pair)
        if kind == 1:
            return remote(p_s.at[c, rows_of((1 - xc) * 2 * unit, 2 * unit), :], h1_s.at[c, 0], xn)
        if kind == 2:
            return remote(p_s.at[c, rows_of(yp + (1 - yc) * 2 * unit, 2 * unit), :], h1_s.at[c, 1], yn)
        if kind == 3:
            return remote(h1_s.at[c, 0, rows_of((1 - yc) * unit, unit), :], h2_s.at[c, 0], yn)
        if kind == 4:
            return remote(h1_s.at[c, 1, rows_of((1 - xc) * unit, unit), :], h2_s.at[c, 1], xn)
        if kind == 5:
            y_of = 1 - yc if f else yc
            r = place(xc * 2 * unit + y_of * unit, unit)
            return remote(r, r, yn)
        if kind == 6:
            x_of = 1 - xc if f else xc
            r = place(yp + yc * 2 * unit + x_of * unit, unit)
            return remote(r, r, xn)
        if kind == 7:
            x_of = 1 - xc if f else xc
            r = place(x_of * 2 * unit, 2 * unit)
            return remote(r, r, xn)
        if kind == 8:
            y_of = 1 - yc if f else yc
            r = place(yp + y_of * 2 * unit, 2 * unit)
            return remote(r, r, yn)
        r = m_ref.at[c, rows_of(half - hb if f else hb, half), :]
        return remote(r, r, pair)

    def taker(f):
        near = (pp == 1) & (f == 0)
        return jnp.where(near, 2, 3), jnp.where(pp == 0, f, jnp.where(near, 0, MOVED[0]))

    def giver(f):
        far = (pp == 3) & (f < MOVED[0])
        return jnp.where(far, 0, 1), jnp.where(far, f, jnp.where(pp == 3, 1, 0))

    def moved_msg(kind, f, arriving=False):
        c = total - moved + f

        def remote(src, dst, there, pp_i, dp_i):
            return pltpu.make_async_remote_copy(src_ref=src, dst_ref=dst, send_sem=mv_send.at[int(kind % 3 > 0), f], recv_sem=mv_recv.at[int(kind % 3 > 0), there], **dev(pp_i, dp_i))
        if kind == 0:
            return remote(m_ref.at[c, rows_of(half - hb, half), :], p_s.at[c], f, pp, pair)
        if kind == 1:
            if arriving:
                return remote(p_s.at[f], p_s.at[f], f, giver(f)[0], dp)
            stage, place = taker(f)
            return remote(p_s.at[c], p_s.at[place], place, stage, dp)
        if kind == 2:
            if arriving:
                return remote(p_s.at[f], m_ref.at[c, rows_of(hb, half), :], f, taker(f)[0], dp)
            stage, piece = giver(f)
            there = total - jnp.where(stage == 0, MOVED[0], MOVED[1]) + piece
            return remote(p_s.at[f], m_ref.at[there, rows_of(hb, half), :], piece, stage, dp)
        r = m_ref.at[c, rows_of(half - hb if arriving else hb, half), :]
        return remote(r, r, f, pp, pair)

    def bytes_of(kind):
        return {0: p_s, 1: h1_s, 3: h2_s, 5: h2_s, 7: h1_s, 9: p_s}[kind].at[0]

    def wait_on(sem, kind):
        place = bytes_of(kind)
        pltpu.make_async_copy(place, place, sem).wait()

    def wait_sent(kind, i):
        j = own_of(i) if kind in (0, 9) else i
        wait_on(send_sem.at[(kind + 1) // 2, j % RING], kind)

    def arrive(kind, i):
        j = own_of(i) if kind in (0, 9) else i
        wait_on(recv_sem.at[(kind + 1) // 2, j % RECV_RING], kind)

    def send(kind, i, foreign):
        if kind >= 3:
            j = own_of(i) if kind == 9 else i

            @pl.when(j >= RING)
            def _():
                wait_sent(kind, i)
        msg(kind, i, foreign).start()
        if kind not in (0, 9):
            msg(kind + 1, i, foreign).start()

    def plus(left, right):
        return (left.astype(F32) + right.astype(F32)).astype(BF16)

    def product(c, slot):
        k, kind, jj = acc_where(c)
        li = (1 - kind) * (1 + jj // COLS)
        ri = (1 - kind) * (jj % COLS) + kind * (COLS + jj)
        right = rm_s[k, ri].reshape(rows4, cw)
        nr = hid // 6 if hid % 768 == 0 else hid // 2
        for n in range(hid // nr):
            r = pl.ds(n * nr, nr)
            g = jnp.dot(lt_s[k, li, r, :], right, preferred_element_type=F32)
            m_ref[c, r, :] = (acc_s[slot, r, :] + g).astype(BF16)

    def produce(i, foreign):
        if foreign:
            return
        c = own_of(i)

        @pl.when(c + AHEAD < own)
        def _():
            acc_start(c + AHEAD, (c + AHEAD) % (AHEAD + 1))
        acc_wait(c % (AHEAD + 1))
        product(c, c % (AHEAD + 1))
        send(0, i, False)

    def stage1(i, foreign):
        if foreign:
            f = i - POS
            moved_msg(1, f, True).wait_recv()
            send(1, i, True)
            return
        c = own_of(i)
        arrive(0, i)
        p_s[c] = plus(p_s[c], m_ref[c, rows_of(hb, half), :])
        send(1, i, False)
        wait_sent(0, i)
        pl.semaphore_signal(free_sem, inc=1, **dev(pp, pair))

    def stage2(i, foreign):
        c = i - POS if foreign else own_of(i)
        arrive(1, i)
        h1_s[c, 0] = plus(h1_s[c, 0], p_s[c, rows_of(xc * 2 * unit, 2 * unit), :])
        h1_s[c, 1] = plus(h1_s[c, 1], p_s[c, rows_of(4 * unit + yc * 2 * unit, 2 * unit), :])
        wait_sent(1, i)
        send(3, i, foreign)
        if not foreign:
            @pl.when(helper & (i < moved))
            def _():
                stage, piece = giver(i)
                pl.semaphore_signal(z_free.at[piece], inc=1, **dev(stage, dp))

    def stage3(i, foreign):
        c = i - POS if foreign else own_of(i)

        def keep(start, value):
            if foreign:
                p_s[c, rows_of(start, unit), :] = value
            else:
                m_ref[c, rows_of(hb + start, unit), :] = value
        arrive(3, i)
        keep(xc * 2 * unit + yc * unit, plus(h1_s[c, 0, rows_of(yc * unit, unit), :], h2_s[c, 0]))
        keep(4 * unit + yc * 2 * unit + xc * unit, plus(h1_s[c, 1, rows_of(xc * unit, unit), :], h2_s[c, 1]))
        send(5, i, foreign)

    def stage4(i, foreign):
        arrive(5, i)
        send(7, i, foreign)

    def stage5(i, foreign):
        arrive(7, i)
        if foreign:
            moved_msg(2, i - POS).start()
            return
        pl.semaphore_wait(free_sem, 1)
        send(9, i, False)

    def stage6(i, foreign):
        if not foreign:
            arrive(9, i)

    plan = ((stage6, 16), (stage5, 14), (stage4, 11), (stage3, 8), (stage2, 5), (stage1, 2), (produce, 0))
    depth = max(lag for _, lag in plan)

    def run(i):
        for fn, lag in plan:
            j = i - lag
            live = (j >= 0) & (j < steps)

            @pl.when(live & jnp.logical_not(is_foreign(j)))
            def _():
                fn(j, False)

            if fn not in (produce, stage6):
                @pl.when(live & is_foreign(j))
                def _():
                    fn(j, True)

    def hand_over(i):
        @pl.when((i >= HAND) & (i < HAND + moved))
        def _():
            f = i - HAND
            c = total - moved + f
            acc_start(c, i % (AHEAD + 1))
            acc_wait(i % (AHEAD + 1))
            product(c, i % (AHEAD + 1))
            moved_msg(0, f).start()

        @pl.when((i >= HAND + 2) & (i < HAND + 2 + moved))
        def _():
            f = i - HAND - 2
            c = total - moved + f
            moved_msg(0, f).wait_recv()
            p_s[c] = plus(p_s[c], m_ref[c, rows_of(hb, half), :])
            moved_msg(0, f).wait_send()
            pl.semaphore_signal(mv_free, inc=1, **dev(pp, pair))
            pl.semaphore_wait(z_free.at[f], 1)
            moved_msg(1, f).start()

    def give(i):
        f = i - (steps + depth - 2 - moved)

        @pl.when((f >= 0) & (f < moved))
        def _():
            moved_msg(2, f, True).wait_recv()
            pl.semaphore_wait(mv_free, 1)
            moved_msg(3, f).start()

    def step(i, carry):
        @pl.when(pp == 0)
        def _():
            @pl.when(i == EARLY[0])
            def _():
                layer(jnp.int32(stages - 1), 1, False)

            @pl.when(i == EARLY[1])
            def _():
                layer(jnp.int32(stages - 1), 0, True)
        run(i)

        @pl.when(jnp.logical_not(helper))
        def _():
            hand_over(i)
            give(i)
        return carry

    @pl.when(pp == 0)
    def _():
        cot_wait(stages - 1)
        keep_cot(stages - 1, 1, cot_now(stages - 1))
    lax.fori_loop(0, steps + depth, step, 0)

    @pl.when(jnp.logical_not(helper))
    def _():
        def take(f, carry):
            moved_msg(3, f, True).wait_recv()
            moved_msg(3, f).wait_send()
            moved_msg(1, f).wait_send()
            return carry
        lax.fori_loop(0, moved, take, 0)

    @pl.when(helper)
    def _():
        def back(f, carry):
            moved_msg(2, f).wait_send()
            return carry
        lax.fori_loop(0, moved, back, 0)

    def drain(i, carry):
        for kind in (3, 5, 7, 9):
            wait_sent(kind, steps - RING + i)
        return carry

    lax.fori_loop(0, RING, drain, 0)

    @pl.when(pp > 0)
    def _():
        cot_wait(stages - 1)

    @pl.when(pp == stages - 1)
    def _():
        cot_wait(stages - 2)

    def sent(t, carry):
        for n in range(TILES):
            cot_copy(t, n).wait_send()
        return carry
    lax.fori_loop(0, stages - pp, sent, 0)
    out_slot = jnp.where(pp == 0, 0, stages - 1)
    for n in range(TILES):
        dx_ref[0, :, n * tile:(n + 1) * tile] = cb_s[out_slot, n]


def write_kernel(sizes, m_ref, dx_ref, gi_ref, go_ref, dxo_ref, out_s, out_sem, dx_sem):
    hid, ff, tok, stages = sizes
    cw = hid // COLS
    nq = ff // cw
    per_layer = 2 * nq
    total = 2 * per_layer
    slots = out_s.shape[0]
    dx_copy = pltpu.make_async_copy(dx_ref, dxo_ref, dx_sem)
    dx_copy.start()

    def copies(c):
        k = 1 - c // per_layer
        b = c % per_layer
        kind, jj = b // nq, b % nq
        slot = c % slots
        a = pltpu.make_async_copy(out_s.at[slot], go_ref.at[0, k, pl.ds(pl.multiple_of((jj // COLS) * hid, 128), hid), pl.ds(pl.multiple_of((jj % COLS) * cw, 128), cw)], out_sem.at[slot])
        b = pltpu.make_async_copy(out_s.at[slot], gi_ref.at[0, k, :, pl.ds(pl.multiple_of(jj * cw, 128), cw)], out_sem.at[slot])
        return kind, a, b

    def body(c, carry):
        @pl.when(c >= slots)
        def _():
            copies(c - slots)[2].wait()
        slot = c % slots
        nr = hid // 4
        for i in range(4):
            r = pl.ds(i * nr, nr)
            out_s[slot, r, :] = m_ref[c, r, :].astype(F32) * 0.125
        kind, a, b = copies(c)

        @pl.when(kind == 0)
        def _():
            a.start()

        @pl.when(kind == 1)
        def _():
            b.start()
        return carry

    lax.fori_loop(0, total, body, 0)

    def drain(i, carry):
        copies(total - slots + i)[2].wait()
        return carry
    lax.fori_loop(0, slots, drain, 0)
    dx_copy.wait()


def solution(mesh):
    stages = mesh.shape['pp']

    def device_fn(w_in, w_out, x_saved, h_saved, dy_in, acc_in, acc_out):
        hid, ff = w_in.shape[2:]
        tok = dy_in.shape[1]
        sizes = (hid, ff, tok, stages)
        cw = hid // COLS
        nq = ff // cw
        total = 4 * nq
        unit = hid // 16
        any_spec = pl.BlockSpec(memory_space=pltpu.HBM)
        vm_spec = pl.BlockSpec(memory_space=pltpu.VMEM)
        m_all, dx = pl.pallas_call(
            functools.partial(main_kernel, sizes),
            out_shape=(pltpu.VMEM((total, hid, cw), BF16), pltpu.VMEM((1, tok, hid), BF16)),
            in_specs=[any_spec] * 7,
            out_specs=(vm_spec, vm_spec),
            scratch_shapes=[
                pltpu.VMEM((2, ff // hid, hid, hid), BF16),
                pltpu.VMEM((2, ff, hid), BF16),
                pltpu.VMEM((2, 1 + ff // hid, hid, stages * tok), BF16),
                pltpu.VMEM((2, COLS + nq, stages, tok, cw), BF16),
                pltpu.VMEM((stages, 2, tok, hid), BF16),
                pltpu.VMEM((stages, TILES, tok, hid // TILES), BF16),
                pltpu.VMEM((AHEAD + 1, hid, cw), F32),
                pltpu.VMEM((total, hid // 2, cw), BF16),
                pltpu.VMEM((total, 2, 2 * unit, cw), BF16),
                pltpu.VMEM((total, 2, unit, cw), BF16),
                pltpu.SemaphoreType.DMA((2, 2)),
                pltpu.SemaphoreType.DMA((stages // 2,)),
                pltpu.SemaphoreType.DMA,
                pltpu.SemaphoreType.DMA,
                pltpu.SemaphoreType.DMA((AHEAD + 1,)),
                pltpu.SemaphoreType.DMA((stages, TILES)),
                pltpu.SemaphoreType.DMA((stages, TILES)),
                pltpu.SemaphoreType.DMA((6, RING)),
                pltpu.SemaphoreType.DMA((6, RECV_RING)),
                pltpu.SemaphoreType.REGULAR,
                pltpu.SemaphoreType.DMA((2, max(MOVED))),
                pltpu.SemaphoreType.DMA((2, max(MOVED))),
                pltpu.SemaphoreType.REGULAR((max(MOVED[:2]),)),
                pltpu.SemaphoreType.REGULAR,
            ],
            compiler_params=pltpu.CompilerParams(collective_id=0, has_side_effects=True, vmem_limit_bytes=46900 * 1024),
            name='chain_reduce',
        )(w_in, w_out, x_saved, h_saved, dy_in, acc_in, acc_out)
        grad_in, grad_out, dx = pl.pallas_call(
            functools.partial(write_kernel, sizes),
            out_shape=(jax.ShapeDtypeStruct((1, 2, hid, ff), F32), jax.ShapeDtypeStruct((1, 2, ff, hid), F32), jax.ShapeDtypeStruct((1, tok, hid), BF16)),
            in_specs=[vm_spec, vm_spec],
            out_specs=(any_spec, any_spec, any_spec),
            scratch_shapes=[pltpu.VMEM((4, hid, cw), F32), pltpu.SemaphoreType.DMA((4,)), pltpu.SemaphoreType.DMA],
            compiler_params=pltpu.CompilerParams(vmem_limit_bytes=16 * 1024 * 1024),
            name='write_out',
        )(m_all, dx)
        return grad_in, grad_out, dx

    return jax.shard_map(device_fn, mesh=mesh, in_specs=(P('pp'), P('pp'), P('pp', None, None, 'dp'), P('pp', None, None, 'dp'), P('pp', 'dp'), P('pp', 'dp'), P('pp', 'dp')), out_specs=(P('pp'), P('pp'), P('pp', 'dp')), check_vma=False)
```
